32 devices in a mesh: rows: 16 (over z, x, core), cols: 2 (over y).
Axes of the slice: x: 2, y: 2, z: 4, core: 2. Of those that a mesh axis runs over, the one named last changes fastest.
Arguments:
- current_frame: bfloat16 [128, 256, 256], P(None, 'rows', 'cols'), may hold values from -6 to 6
- history_frames: bfloat16 [3, 128, 256, 256], P(None, None, 'rows', 'cols'), may hold values from -6 to 6
- offsets: int32 [3, 2], replicated, may hold values from -16 to 16, as said below
- compress_weight: bfloat16 [32, 128], replicated, may hold values from -0.5 to 0.5
- mixer_weight: bfloat16 [3, 3, 128, 224], replicated, may hold values from -0.125 to 0.125
- mixer_bias: float32 [128], replicated, may hold values from -3 to 3
Outputs:
- joined_grid: bfloat16 [128, 256, 256], P(None, 'rows', 'cols')
The draws below stay inside these ranges and needn't reach their ends.
Inputs may be any that keep to these rules, and one draw needn't show every extreme that they name: offsets[k, 0] lies in -8..8 and offsets[k, 1] in -16..16; no offset is 0; in each of the two columns one frame's offset equals the bound and another equals its negative.
All inputs are finite; a program needn't handle non-finite values.
Results may differ from the reference program's by a relative error of at most 0.0034.
Values may be sent and summed in bfloat16 or wider, within the bound.
A program may use at most 64 MiB of HBM per device.

```python
import jax
import jax.numpy as jnp
from jax import lax

C = 128
CP = 32
FRAMES = 3
CR = 16
SHIFT_X = 16
SHIFT_Y = 8
GRID_ROWS = 256
GRID_COLS = 256


def offset_column(key, bound):
    key_mags, key_sign, key_perm = jax.random.split(key, 3)
    spare_mag = jax.random.randint(key_mags, (), 1, bound + 1)
    mags = jnp.stack([jnp.int32(bound), jnp.int32(bound), spare_mag.astype(jnp.int32)])
    spare = 2 * jax.random.randint(key_sign, (), 0, 2) - 1
    signs = jnp.stack([jnp.int32(1), jnp.int32(-1), spare.astype(jnp.int32)])
    order = jax.random.permutation(key_perm, jnp.arange(3, dtype=jnp.int32))
    return (mags * signs)[order]


def draw_offsets(key, part):
    key_rows = jax.random.fold_in(key, 11)
    key_cols = jax.random.fold_in(key, 23)
    return jnp.stack([offset_column(key_rows, SHIFT_Y), offset_column(key_cols, SHIFT_X)], axis=1).astype(jnp.int32)


def block_scale(stream_key, extent, shards, low, largest):
    gain = 1.0
    for axis_at, parts in shards:
        draws = jax.random.uniform(jax.random.fold_in(jax.random.fold_in(stream_key, 6), axis_at), (parts,), jnp.float32, low / len(shards), largest / len(shards))
        gain = gain * jnp.repeat(jnp.exp(draws), extent[axis_at] // parts).reshape((-1,) + (1,) * (len(extent) - 1 - axis_at))
    return gain


def noise(key, dims, scale, reach, cuts=(), kind=jnp.bfloat16):
    drawn = scale * jax.random.normal(key, dims, jnp.float32)
    if cuts:
        drawn = drawn * block_scale(key, dims, cuts, -0.22, 0.18)
    return jnp.clip(drawn, -reach, reach).astype(kind)


def setup_inputs(seed: int = 0) -> dict:
    key_list = jax.random.split(jax.random.key(seed), 7)
    return {
        "current_frame": noise(key_list[0], (C, GRID_ROWS, GRID_COLS), 1.0, 6.0, ((1, 16), (2, 2))),
        "history_frames": noise(key_list[1], (FRAMES, C, GRID_ROWS, GRID_COLS), 1.0, 6.0, ((2, 16), (3, 2))),
        "offsets": draw_offsets(jax.random.fold_in(key_list[6], 71), 0),
        "compress_weight": noise(key_list[3], (CP, C), C ** -0.5, 0.5),
        "mixer_weight": noise(key_list[4], (3, 3, C, C + FRAMES * CP), (9 * (C + FRAMES * CP)) ** -0.5, 0.125),
        "mixer_bias": noise(key_list[5], (C,), 0.5, 3.0, (), jnp.float32),
    }


def shift_frame(frame, row_offset, col_offset):
    padded = jnp.pad(frame, ((0, 0), (SHIFT_Y, SHIFT_Y), (SHIFT_X, SHIFT_X)))
    starts = (jnp.int32(0), (SHIFT_Y - row_offset).astype(jnp.int32), (SHIFT_X - col_offset).astype(jnp.int32))
    return lax.dynamic_slice(padded, starts, (CP, GRID_ROWS, GRID_COLS))


def conv_taps(present_rows, older_rows, mixer_weight, mixer_bias):
    height = present_rows.shape[1] - 2
    width = present_rows.shape[2] - 2
    channels = present_rows.shape[0]
    total = jnp.zeros((mixer_weight.shape[2], height * width), jnp.float32)
    for tap_row in range(3):
        for tap_col in range(3):
            present = present_rows[:, tap_row:tap_row + height, tap_col:tap_col + width].reshape(channels, -1)
            older = older_rows[:, tap_row:tap_row + height, tap_col:tap_col + width].reshape(older_rows.shape[0], -1)
            total = total + jnp.dot(mixer_weight[tap_row, tap_col, :, :channels], present, preferred_element_type=jnp.float32)
            total = total + jnp.dot(mixer_weight[tap_row, tap_col, :, channels:], older, preferred_element_type=jnp.float32)
    result = jnp.maximum(total + mixer_bias[:, None], 0.0)
    return result.astype(jnp.bfloat16).reshape(-1, height, width)


def reference(current_frame, history_frames, offsets, compress_weight, mixer_weight, mixer_bias):
    pieces = []
    for frame_index in range(FRAMES):
        flattened = history_frames[frame_index].reshape(C, -1)
        reduced = jnp.dot(compress_weight, flattened, preferred_element_type=jnp.float32).astype(jnp.bfloat16)
        reduced = reduced.reshape(CP, GRID_ROWS, GRID_COLS)
        pieces.append(shift_frame(reduced, offsets[frame_index, 0], offsets[frame_index, 1]))
    shifted = jnp.concatenate(pieces, axis=0)
    present_pad = jnp.pad(current_frame, ((0, 0), (1, 1), (1, 1)))
    older_pad = jnp.pad(shifted, ((0, 0), (1, 1), (1, 1)))

    def row_block(block_index):
        row_start = (block_index * CR).astype(jnp.int32)
        present_rows = lax.dynamic_slice_in_dim(present_pad, row_start, CR + 2, 1)
        older_rows = lax.dynamic_slice_in_dim(older_pad, row_start, CR + 2, 1)
        return conv_taps(present_rows, older_rows, mixer_weight, mixer_bias)

    blocks = lax.map(row_block, jnp.arange(GRID_ROWS // CR, dtype=jnp.int32))
    return blocks.transpose(1, 0, 2, 3).reshape(C, GRID_ROWS, GRID_COLS)
```

```python
import functools

import jax
import jax.numpy as jnp
from jax import lax
from jax.experimental import pallas as pl
from jax.experimental.pallas import tpu as pltpu
from jax.sharding import PartitionSpec as P

MESH = pl.DeviceIdType.MESH
BF = jnp.bfloat16
F32 = jnp.float32
SEG = 32


def pick(ds, positive):
    n = len(ds)
    first, last = jnp.int32(n - 1), jnp.int32(0)
    for k in range(n):
        hit = ds[k] > 0 if positive else ds[k] < 0
        last = jnp.where(hit, jnp.int32(k), last)
    for k in reversed(range(n)):
        hit = ds[k] > 0 if positive else ds[k] < 0
        first = jnp.where(hit, jnp.int32(k), first)
    return first, last


def kernel(
    nr, nc,
    off, hist_hbm, cur_hbm, mix_hbm, cw_ref, bias_ref, out_ref,
    hist, cur, mix, red, rows_all, vsend, hsend, hrecv, csend, cols_all,
    qsend, qrecv, pk, pkrecv, sp, ss, acc, outs, lsem, ssem, rsem,
):
    frames, ch, h, w = hist.shape
    cp = cw_ref.shape[0]
    depth = frames * cp
    reach = h // 2 + 1
    groups = h // 4
    cg = -(-reach // 4)
    own = frames * h
    va, vb = own, own + 2 * reach
    ha, hb = 0, 2 * groups
    ca, cb = 4 * groups, 4 * groups + 2 * cg
    pb, sb = 3 * ch, 3 * depth

    r = lax.axis_index("rows")
    c = lax.axis_index("cols")
    has_up, has_dn, has_lf, has_rt = r > 0, r < nr - 1, c > 0, c < nc - 1
    up_dev, dn_dev, lf_dev, rt_dev = (r - 1, c), (r + 1, c), (r, c - 1), (r, c + 1)

    loads = [pltpu.make_async_copy(hist_hbm.at[k], hist.at[k], lsem.at[k]) for k in range(frames)]
    load_cur = pltpu.make_async_copy(cur_hbm, cur, lsem.at[frames])
    load_mix = pltpu.make_async_copy(mix_hbm, mix, lsem.at[frames + 1])
    for x in (*loads, load_cur, load_mix):
        x.start()

    barrier = pltpu.get_barrier_semaphore()
    for cond, dev in ((has_up, up_dev), (has_dn, dn_dev), (has_lf, lf_dev), (has_rt, rt_dev)):
        @pl.when(cond)
        def _(dev=dev):
            pl.semaphore_signal(barrier, inc=1, device_id=dev, device_id_type=MESH)

    def remote(n, d, src, dst, sideways):
        dev = ((rt_dev, lf_dev) if sideways else (dn_dev, up_dev))[d]
        copy = pltpu.make_async_remote_copy(
            src_ref=src, dst_ref=dst, send_sem=ssem.at[n, d], recv_sem=rsem.at[n, d],
            device_id=dev, device_id_type=MESH,
        )
        ways = (has_rt, has_lf) if sideways else (has_dn, has_up)
        return copy, ways[d], ways[1 - d]

    def start(copies):
        for copy, sends, _ in copies:
            @pl.when(sends)
            def _(copy=copy):
                copy.start()

    def arrive(copies):
        for copy, _, comes in copies:
            @pl.when(comes)
            def _(copy=copy):
                copy.wait_recv()

    def finish(copies):
        for copy, sends, _ in copies:
            @pl.when(sends)
            def _(copy=copy):
                copy.wait_send()

    hcopy = [remote(0, d, hsend.at[d], hrecv.at[pl.ds((ha, hb)[d], 2 * groups)], True) for d in (0, 1)]
    vcopy = [remote(1, d, vsend.at[d], rows_all.at[pl.ds((va, vb)[d], 2 * reach)], False) for d in (0, 1)]
    qcopy = [remote(2, d, qsend, qrecv.at[d], True) for d in (0, 1)]
    pcopy = [
        remote(3, 0, sp.at[pl.ds(h * pb + ch, ch)], sp.at[pl.ds(ch, ch)], False),
        remote(3, 1, sp.at[pl.ds(pb + ch, ch)], sp.at[pl.ds((h + 1) * pb + ch, ch)], False),
    ]
    ccopy = [remote(4, d, csend.at[d], cols_all.at[pl.ds((ca, cb)[d], 2 * cg)], False) for d in (0, 1)]
    kcopy = [remote(5, d, pk, pkrecv.at[d], False) for d in (0, 1)]

    dys = [off[k, 0] for k in range(frames)]
    dxs = [off[k, 1] for k in range(frames)]
    down, up = pick(dys, True), pick(dys, False)
    right, left = pick(dxs, True), pick(dxs, False)

    def slot(k, d, plus, minus):
        other = jnp.where(d > 0, plus[0], minus[0]) != k
        return jnp.where(other, jnp.int32(1), jnp.int32(0))

    vslot = [slot(k, dys[k], down, up) for k in range(frames)]
    hslot = [slot(k, dxs[k], right, left) for k in range(frames)]
    side = [jnp.where(dxs[k] > 0, ha, hb) + hslot[k] * groups for k in range(frames)]

    def clear(ref, first, size):
        ref[pl.ds(first, size)] = jnp.zeros((size, *ref.shape[1:]), BF)

    @pl.when(r == 0)
    def _():
        clear(rows_all, va, 2 * reach)
        clear(cols_all, ca, 2 * cg)
        clear(pkrecv, 0, 1)
        clear(sp, ch, ch)

    @pl.when(r == nr - 1)
    def _():
        clear(rows_all, vb, 2 * reach)
        clear(cols_all, cb, 2 * cg)
        clear(pkrecv, 1, 1)
        clear(sp, (h + 1) * pb + ch, ch)

    @pl.when(c == 0)
    def _():
        clear(hrecv, ha, 2 * groups)
        clear(qrecv, 0, 1)

    @pl.when(c == nc - 1)
    def _():
        clear(hrecv, hb, 2 * groups)
        clear(qrecv, 1, 1)

    for k in range(frames):
        loads[k].wait()
        rows = jnp.swapaxes(hist[k], 0, 1)
        for y in range(0, h, 2):
            rhs = jnp.concatenate([rows[y], rows[y + 1]], axis=1)
            got = jnp.dot(cw_ref[...], rhs, preferred_element_type=F32).astype(BF)
            for e in (0, 1):
                part = got[:, e * w:(e + 1) * w]
                red[k * h + y + e] = part
                rows_all[k * h + y + e] = part

    lane = lax.broadcasted_iota(jnp.int32, (cp, w), 1)
    for d in (0, 1):
        for s in (0, 1):
            frame, base = (right[s], SEG) if d == 0 else (left[s], 0)
            for g in range(groups):
                tile = None
                for q in range(4):
                    row = red[frame * h + 4 * g + q]
                    turn = (base + SEG * q) % w
                    row = pltpu.roll(row, turn, 1) if turn else row
                    tile = row if tile is None else jnp.where(lane >= SEG * q, row, tile)
                hsend[d, s * groups + g] = tile

    count = sum(jnp.where(x, jnp.int32(1), jnp.int32(0)) for x in (has_up, has_dn, has_lf, has_rt))
    pl.semaphore_wait(barrier, count)
    start(hcopy)
    for s in (0, 1):
        vsend[0, pl.ds(s * reach, reach)] = red[pl.ds(down[s] * h + h - reach, reach)]
        vsend[1, pl.ds(s * reach, reach)] = red[pl.ds(up[s] * h, reach)]
    start(vcopy)

    load_cur.wait()
    rows = jnp.swapaxes(cur[...], 0, 1)
    for y in range(h):
        sp[pl.ds((y + 1) * pb + ch, ch)] = rows[y]
    start(pcopy)
    lane_c = lax.broadcasted_iota(jnp.int32, (ch, w), 1)
    tile = jnp.zeros((ch, w), BF)
    for t in range(1, h + 1):
        turned = pltpu.roll(rows[t - 1], 2 * t + 2, 1)
        tile = jnp.where((lane_c >= 2 * t + 1) & (lane_c <= 2 * t + 2), turned, tile)
    qsend[...] = tile
    start(qcopy)

    load_mix.wait()
    wp = jnp.concatenate([mix[i, j, :, :ch] for i in range(3) for j in range(3)], axis=1)
    fill = jnp.zeros((ch, w - depth), BF)
    taps = [jnp.concatenate([mix[i, j, :, ch:], fill], axis=1) for i in range(3) for j in range(3)]
    extra = [(tap, f) for tap in (6, 7) for f in range(frames)]
    tiles, order = [], []
    for n in range(6):
        tap, f = extra[n]
        turned = pltpu.roll(taps[tap], w - cp - f * cp, 1)
        tiles.append(jnp.where(lane_c >= depth, turned, taps[n]))
        order += [(n, g) for g in range(frames)] + [(tap, f)]
    tiles.append(taps[8])
    order += [(8, g) for g in range(frames)] + [(8, 0)]
    ws = jnp.concatenate(tiles, axis=1)
    wide = jnp.broadcast_to(bias_ref[...][None, :], (ch, ch))
    eye = lax.broadcasted_iota(jnp.int32, (ch, ch), 0) == lax.broadcasted_iota(jnp.int32, (ch, ch), 1)
    bias = jnp.sum(jnp.where(eye, wide, 0.0), axis=1, keepdims=True)

    arrive(qcopy)
    edge = jnp.where((lane_c & 1) == 1, qrecv[0], pltpu.roll(qrecv[1], w - 2, 1))
    pk[...] = edge
    start(kcopy)
    arrive(hcopy)
    for s in (0, 1):
        for d, frame in ((0, down[s]), (1, up[s])):
            base = jnp.int32(0)
            for k in range(frames):
                base = jnp.where(frame == k, side[k], base)
            first = base + (groups - cg if d == 0 else 0)
            csend[d, pl.ds(s * cg, cg)] = hrecv[pl.ds(first, cg)]
    start(ccopy)
    cols_all[pl.ds(0, 4 * groups)] = hrecv[...]

    def widen(t, edge):
        mid = sp[pl.ds(t * pb + ch, ch)]
        ends = pltpu.roll(edge, w - 2 * t - 1, 1)
        sp[pl.ds(t * pb, ch)] = jnp.where(lane_c == 0, ends, pltpu.roll(mid, 1, 1))
        sp[pl.ds(t * pb + 2 * ch, ch)] = jnp.where(lane_c == w - 1, ends, pltpu.roll(mid, w - 1, 1))

    def present(p):
        y = 2 * p
        rhs = jnp.concatenate([sp[pl.ds(y * pb, 3 * pb)], sp[pl.ds((y + 1) * pb, 3 * pb)]], axis=1)
        acc[p] = jnp.dot(wp, rhs, preferred_element_type=F32)

    for t in range(1, h + 1):
        widen(t, edge)
    for p in range(1, h // 2 - 1):
        present(p)
    arrive(pcopy)
    arrive(kcopy)
    edge = jnp.where(
        lane_c < 2, pltpu.roll(pkrecv[0], w - 2 * h, 1), pltpu.roll(pkrecv[1], 2 * h, 1)
    )
    widen(0, edge)
    widen(h + 1, edge)
    present(0)
    present(h // 2 - 1)

    arrive(vcopy)
    arrive(ccopy)
    for k in range(frames):
        dy, dx = dys[k], dxs[k]
        plus = dx > 0
        lo = jnp.where(plus, 0, w + dx)
        hi = jnp.where(plus, dx, w)
        flag = jnp.where(plus, jnp.int32(1), jnp.int32(0))
        base = jnp.where((lane >= lo) & (lane < hi), jnp.int32(1), jnp.int32(0))
        mid_m = base == 1
        lo_m = jnp.where(lane == w - 1, flag, base) == 1
        hi_m = jnp.where(lane == 0, 1 - flag, base) == 1
        lf_out = (lane == 0) & (c == 0)
        rt_out = (lane == w - 1) & (c == nc - 1)
        own_turn = lax.rem(dx + w, w)
        halo_turn = dx - jnp.where(plus, SEG, 0)
        for t in range(h + 2):
            y = t - 1 - dy
            above, below = y < 0, y >= h
            at = jnp.where(
                above, va + vslot[k] * reach + y + reach,
                jnp.where(below, vb + vslot[k] * reach + y - h, k * h + y),
            )
            near = jnp.where(above, y + h, jnp.where(below, y - h, y))
            quad = lax.shift_right_logical(near, jnp.int32(2))
            col = jnp.where(
                above, ca + vslot[k] * cg + quad - (groups - cg),
                jnp.where(below, cb + vslot[k] * cg + quad, side[k] + quad),
            )
            turn = lax.rem(halo_turn - SEG * (near & 3) + 2 * w, w)
            mine = pltpu.roll(rows_all[at], own_turn, 1)
            theirs = pltpu.roll(cols_all[col], turn, 1)
            place = t * sb + k * cp
            lf = pltpu.roll(jnp.where(lo_m, theirs, mine), 1, 1)
            rt = pltpu.roll(jnp.where(hi_m, theirs, mine), w - 1, 1)
            ss[pl.ds(place, cp)] = jnp.where(lf_out, jnp.zeros_like(lf), lf)
            ss[pl.ds(place + depth, cp)] = jnp.where(mid_m, theirs, mine)
            ss[pl.ds(place + 2 * depth, cp)] = jnp.where(rt_out, jnp.zeros_like(rt), rt)

    @pl.when(r == 0)
    def _():
        clear(ss, 0, sb)

    @pl.when(r == nr - 1)
    def _():
        clear(ss, (h + 1) * sb, sb)

    for p in range(h // 2):
        halves = []
        for y in (2 * p, 2 * p + 1):
            halves.append(jnp.concatenate(
                [ss[pl.ds((y + tap // 3) * sb + (tap % 3) * depth + f * cp, cp)] for tap, f in order], axis=0
            ))
        total = acc[p] + jnp.dot(ws, jnp.concatenate(halves, axis=1), preferred_element_type=F32)
        total = jnp.maximum(total + bias, 0.0).astype(BF)
        outs[2 * p] = total[:, :w]
        outs[2 * p + 1] = total[:, w:]
    out_ref[...] = jnp.swapaxes(outs[...], 0, 1)

    for copies in (hcopy, vcopy, qcopy, pcopy, ccopy, kcopy):
        finish(copies)


def body(nr, nc, current_frame, history_frames, offsets, compress_weight, mixer_weight, mixer_bias):
    frames, ch, h, w = history_frames.shape
    cp = compress_weight.shape[0]
    depth = frames * cp
    reach = h // 2 + 1
    groups = h // 4
    cg = -(-reach // 4)
    anyspace = pl.BlockSpec(memory_space=pl.ANY)
    vmem = pl.BlockSpec(memory_space=pltpu.VMEM)
    return pl.pallas_call(
        functools.partial(kernel, nr, nc),
        out_shape=jax.ShapeDtypeStruct((ch, h, w), BF),
        in_specs=[pl.BlockSpec(memory_space=pltpu.SMEM), anyspace, anyspace, anyspace, vmem, vmem],
        out_specs=vmem,
        scratch_shapes=[
            pltpu.VMEM((frames, ch, h, w), BF),
            pltpu.VMEM((ch, h, w), BF),
            pltpu.VMEM(mixer_weight.shape, BF),
            pltpu.VMEM((frames * h, cp, w), BF),
            pltpu.VMEM((frames * h + 4 * reach, cp, w), BF),
            pltpu.VMEM((2, 2 * reach, cp, w), BF),
            pltpu.VMEM((2, 2 * groups, cp, w), BF),
            pltpu.VMEM((4 * groups, cp, w), BF),
            pltpu.VMEM((2, 2 * cg, cp, w), BF),
            pltpu.VMEM((4 * groups + 4 * cg, cp, w), BF),
            pltpu.VMEM((ch, w), BF),
            pltpu.VMEM((2, ch, w), BF),
            pltpu.VMEM((ch, w), BF),
            pltpu.VMEM((2, ch, w), BF),
            pltpu.VMEM(((h + 2) * 3 * ch, w), BF),
            pltpu.VMEM(((h + 2) * 3 * depth, w), BF),
            pltpu.VMEM((h // 2, ch, 2 * w), F32),
            pltpu.VMEM((h, ch, w), BF),
            pltpu.SemaphoreType.DMA((frames + 2,)),
            pltpu.SemaphoreType.DMA((6, 2)),
            pltpu.SemaphoreType.DMA((6, 2)),
        ],
        compiler_params=pltpu.CompilerParams(collective_id=0, has_side_effects=True),
        name="join",
    )(offsets, history_frames, current_frame, mixer_weight, compress_weight, mixer_bias)


def solution(mesh):
    in_specs = (P(None, "rows", "cols"), P(None, None, "rows", "cols"), P(), P(), P(), P())
    out_specs = P(None, "rows", "cols")
    return jax.shard_map(
        functools.partial(body, mesh.shape["rows"], mesh.shape["cols"]),
        mesh=mesh, in_specs=in_specs, out_specs=out_specs, check_vma=False,
    )
```

```python
import functools

import jax
import jax.numpy as jnp
from jax import lax
from jax.experimental import pallas as pl
from jax.experimental.pallas import tpu as pltpu
from jax.sharding import PartitionSpec as P

MESH = pl.DeviceIdType.MESH
BF = jnp.bfloat16
F32 = jnp.float32
SEG = 32


def pick(ds, positive):
    n = len(ds)
    first, last = jnp.int32(n - 1), jnp.int32(0)
    for k in range(n):
        hit = ds[k] > 0 if positive else ds[k] < 0
        last = jnp.where(hit, jnp.int32(k), last)
    for k in reversed(range(n)):
        hit = ds[k] > 0 if positive else ds[k] < 0
        first = jnp.where(hit, jnp.int32(k), first)
    return first, last


def kernel(
    nr, nc,
    off, hist_hbm, cur_hbm, mix_hbm, cw_ref, bias_ref, out_ref,
    hist, cur, mix, red, rows_all, vsend, hsend, hrecv, csend, cols_all,
    qsend, qrecv, pk, pkrecv, sp, ss, acc, wp, ws, lsem, ssem, rsem,
):
    frames, ch, h, w = hist.shape
    cp = cw_ref.shape[0]
    depth = frames * cp
    reach = h // 2 + 1
    groups = h // 4
    cg = -(-reach // 4)
    own = frames * h
    va, vb = own, own + 2 * reach
    ha, hb = 0, 2 * groups
    ca, cb = 4 * groups, 4 * groups + 2 * cg
    pb, sb = 3 * ch, 3 * depth

    r = lax.axis_index("rows")
    c = lax.axis_index("cols")
    has_up, has_dn, has_lf, has_rt = r > 0, r < nr - 1, c > 0, c < nc - 1
    up_dev, dn_dev, lf_dev, rt_dev = (r - 1, c), (r + 1, c), (r, c - 1), (r, c + 1)

    loads = [pltpu.make_async_copy(hist_hbm.at[k], hist.at[k], lsem.at[k]) for k in range(frames)]
    load_cur = pltpu.make_async_copy(cur_hbm, cur, lsem.at[frames])
    load_mix = pltpu.make_async_copy(mix_hbm, mix, lsem.at[frames + 1])
    for x in (*loads, load_cur, load_mix):
        x.start()

    barrier = pltpu.get_barrier_semaphore()
    for cond, dev in ((has_up, up_dev), (has_dn, dn_dev), (has_lf, lf_dev), (has_rt, rt_dev)):
        @pl.when(cond)
        def _(dev=dev):
            pl.semaphore_signal(barrier, inc=1, device_id=dev, device_id_type=MESH)

    def remote(n, d, src, dst, sideways):
        dev = ((rt_dev, lf_dev) if sideways else (dn_dev, up_dev))[d]
        copy = pltpu.make_async_remote_copy(
            src_ref=src, dst_ref=dst, send_sem=ssem.at[n, d], recv_sem=rsem.at[n, d],
            device_id=dev, device_id_type=MESH,
        )
        ways = (has_rt, has_lf) if sideways else (has_dn, has_up)
        return copy, ways[d], ways[1 - d]

    def start(copies):
        for copy, sends, _ in copies:
            @pl.when(sends)
            def _(copy=copy):
                copy.start()

    def arrive(copies):
        for copy, _, comes in copies:
            @pl.when(comes)
            def _(copy=copy):
                copy.wait_recv()

    def finish(copies):
        for copy, sends, _ in copies:
            @pl.when(sends)
            def _(copy=copy):
                copy.wait_send()

    hcopy = [remote(0, d, hsend.at[d], hrecv.at[pl.ds((ha, hb)[d], 2 * groups)], True) for d in (0, 1)]
    vcopy = [remote(1, d, vsend.at[d], rows_all.at[pl.ds((va, vb)[d], 2 * reach)], False) for d in (0, 1)]
    qcopy = [remote(2, d, qsend, qrecv.at[d], True) for d in (0, 1)]
    pcopy = [
        remote(3, 0, sp.at[pl.ds(h * pb + ch, ch)], sp.at[pl.ds(ch, ch)], False),
        remote(3, 1, sp.at[pl.ds(pb + ch, ch)], sp.at[pl.ds((h + 1) * pb + ch, ch)], False),
    ]
    ccopy = [remote(4, d, csend.at[d], cols_all.at[pl.ds((ca, cb)[d], 2 * cg)], False) for d in (0, 1)]
    kcopy = [remote(5, d, pk, pkrecv.at[d], False) for d in (0, 1)]

    dys = [off[0, k] for k in range(frames)]
    dxs = [off[1, k] for k in range(frames)]
    down, up = pick(dys, True), pick(dys, False)
    right, left = pick(dxs, True), pick(dxs, False)

    def slot(k, d, plus, minus):
        other = jnp.where(d > 0, plus[0], minus[0]) != k
        return jnp.where(other, jnp.int32(1), jnp.int32(0))

    vslot = [slot(k, dys[k], down, up) for k in range(frames)]
    hslot = [slot(k, dxs[k], right, left) for k in range(frames)]
    side = [jnp.where(dxs[k] > 0, ha, hb) + hslot[k] * groups for k in range(frames)]

    def clear(ref, first, size):
        ref[pl.ds(first, size)] = jnp.zeros((size, *ref.shape[1:]), BF)

    @pl.when(r == 0)
    def _():
        clear(rows_all, va, 2 * reach)
        clear(cols_all, ca, 2 * cg)
        clear(pkrecv, 0, 1)
        clear(sp, ch, ch)

    @pl.when(r == nr - 1)
    def _():
        clear(rows_all, vb, 2 * reach)
        clear(cols_all, cb, 2 * cg)
        clear(pkrecv, 1, 1)
        clear(sp, (h + 1) * pb + ch, ch)

    @pl.when(c == 0)
    def _():
        clear(hrecv, ha, 2 * groups)
        clear(qrecv, 0, 1)

    @pl.when(c == nc - 1)
    def _():
        clear(hrecv, hb, 2 * groups)
        clear(qrecv, 1, 1)

    for k in range(frames):
        loads[k].wait()
        rows = jnp.swapaxes(hist[k], 0, 1)
        for y in range(0, h, 2):
            rhs = jnp.concatenate([rows[y], rows[y + 1]], axis=1)
            got = jnp.dot(cw_ref[...], rhs, preferred_element_type=F32).astype(BF)
            for e in (0, 1):
                part = got[:, e * w:(e + 1) * w]
                red[k * h + y + e] = part
                rows_all[k * h + y + e] = part

    lane = lax.broadcasted_iota(jnp.int32, (cp, w), 1)
    for d in (0, 1):
        for s in (0, 1):
            frame, base = (right[s], SEG) if d == 0 else (left[s], 0)
            for g in range(groups):
                tile = None
                for q in range(4):
                    row = red[frame * h + 4 * g + q]
                    turn = (base + SEG * q) % w
                    row = pltpu.roll(row, turn, 1) if turn else row
                    tile = row if tile is None else jnp.where(lane >= SEG * q, row, tile)
                hsend[d, s * groups + g] = tile

    count = sum(jnp.where(x, jnp.int32(1), jnp.int32(0)) for x in (has_up, has_dn, has_lf, has_rt))
    pl.semaphore_wait(barrier, count)
    start(hcopy)
    for s in (0, 1):
        vsend[0, pl.ds(s * reach, reach)] = red[pl.ds(down[s] * h + h - reach, reach)]
        vsend[1, pl.ds(s * reach, reach)] = red[pl.ds(up[s] * h, reach)]
    start(vcopy)

    load_cur.wait()
    rows = jnp.swapaxes(cur[...], 0, 1)
    for y in range(h):
        sp[pl.ds((y + 1) * pb + ch, ch)] = rows[y]
    start(pcopy)
    lane_c = lax.broadcasted_iota(jnp.int32, (ch, w), 1)
    tile = jnp.zeros((ch, w), BF)
    for t in range(1, h + 1):
        turned = pltpu.roll(rows[t - 1], 2 * t + 2, 1)
        tile = jnp.where((lane_c >= 2 * t + 1) & (lane_c <= 2 * t + 2), turned, tile)
    qsend[...] = tile
    start(qcopy)

    load_mix.wait()
    for i in range(3):
        for j in range(3):
            wp[:, (3 * i + j) * ch:(3 * i + j + 1) * ch] = jnp.swapaxes(mix[i, j, :ch], 0, 1)
    past = [mix[i, j, ch:] for i in range(3) for j in range(3)]
    past.append(jnp.zeros((ws.shape[1] - 9 * depth, ch), BF))
    past = jnp.concatenate(past, axis=0)
    for n in range(0, ws.shape[1], ch):
        ws[:, n:n + ch] = jnp.swapaxes(past[n:n + ch], 0, 1)
    wide = jnp.broadcast_to(bias_ref[...][None, :], (ch, ch))
    eye = lax.broadcasted_iota(jnp.int32, (ch, ch), 0) == lax.broadcasted_iota(jnp.int32, (ch, ch), 1)
    bias = jnp.sum(jnp.where(eye, wide, 0.0), axis=1, keepdims=True)

    arrive(qcopy)
    edge = jnp.where((lane_c & 1) == 1, qrecv[0], pltpu.roll(qrecv[1], w - 2, 1))
    pk[...] = edge
    start(kcopy)
    arrive(hcopy)
    for s in (0, 1):
        for d, frame in ((0, down[s]), (1, up[s])):
            base = jnp.int32(0)
            for k in range(frames):
                base = jnp.where(frame == k, side[k], base)
            first = base + (groups - cg if d == 0 else 0)
            csend[d, pl.ds(s * cg, cg)] = hrecv[pl.ds(first, cg)]
    start(ccopy)
    cols_all[pl.ds(0, 4 * groups)] = hrecv[...]

    def widen(t, edge):
        mid = sp[pl.ds(t * pb + ch, ch)]
        ends = pltpu.roll(edge, w - 2 * t - 1, 1)
        sp[pl.ds(t * pb, ch)] = jnp.where(lane_c == 0, ends, pltpu.roll(mid, 1, 1))
        sp[pl.ds(t * pb + 2 * ch, ch)] = jnp.where(lane_c == w - 1, ends, pltpu.roll(mid, w - 1, 1))

    def present(p):
        y = 2 * p
        rhs = jnp.concatenate([sp[pl.ds(y * pb, 3 * pb)], sp[pl.ds((y + 1) * pb, 3 * pb)]], axis=1)
        acc[p] = jnp.dot(wp[...], rhs, preferred_element_type=F32)

    for t in range(1, h + 1):
        widen(t, edge)
    for p in range(1, h // 2 - 1):
        present(p)
    arrive(pcopy)
    arrive(kcopy)
    edge = jnp.where(
        lane_c < 2, pltpu.roll(pkrecv[0], w - 2 * h, 1), pltpu.roll(pkrecv[1], 2 * h, 1)
    )
    widen(0, edge)
    widen(h + 1, edge)
    present(0)
    present(h // 2 - 1)

    arrive(vcopy)
    arrive(ccopy)
    for k in range(frames):
        dy, dx = dys[k], dxs[k]
        plus = dx > 0
        lo = jnp.where(plus, 0, w + dx)
        hi = jnp.where(plus, dx, w)
        flag = jnp.where(plus, jnp.int32(1), jnp.int32(0))
        base = jnp.where((lane >= lo) & (lane < hi), jnp.int32(1), jnp.int32(0))
        mid_m = base == 1
        lo_m = jnp.where(lane == w - 1, flag, base) == 1
        hi_m = jnp.where(lane == 0, 1 - flag, base) == 1
        lf_out = (lane == 0) & (c == 0)
        rt_out = (lane == w - 1) & (c == nc - 1)
        own_turn = lax.rem(dx + w, w)
        halo_turn = dx - jnp.where(plus, SEG, 0)
        for t in range(h + 2):
            y = t - 1 - dy
            above, below = y < 0, y >= h
            at = jnp.where(
                above, va + vslot[k] * reach + y + reach,
                jnp.where(below, vb + vslot[k] * reach + y - h, k * h + y),
            )
            near = jnp.where(above, y + h, jnp.where(below, y - h, y))
            quad = lax.shift_right_logical(near, jnp.int32(2))
            col = jnp.where(
                above, ca + vslot[k] * cg + quad - (groups - cg),
                jnp.where(below, cb + vslot[k] * cg + quad, side[k] + quad),
            )
            turn = lax.rem(halo_turn - SEG * (near & 3) + 2 * w, w)
            mine = pltpu.roll(rows_all[at], own_turn, 1)
            theirs = pltpu.roll(cols_all[col], turn, 1)
            place = t * sb + k * cp
            lf = pltpu.roll(jnp.where(lo_m, theirs, mine), 1, 1)
            rt = pltpu.roll(jnp.where(hi_m, theirs, mine), w - 1, 1)
            ss[pl.ds(place, cp)] = jnp.where(lf_out, jnp.zeros_like(lf), lf)
            ss[pl.ds(place + depth, cp)] = jnp.where(mid_m, theirs, mine)
            ss[pl.ds(place + 2 * depth, cp)] = jnp.where(rt_out, jnp.zeros_like(rt), rt)

    @pl.when(r == 0)
    def _():
        clear(ss, 0, sb)

    @pl.when(r == nr - 1)
    def _():
        clear(ss, (h + 1) * sb, sb)

    lead = ws.shape[1] - 9 * depth
    for p in range(h // 2):
        halves = []
        for y in (2 * p, 2 * p + 1):
            rows = ss[pl.ds(y * sb, 3 * sb)]
            halves.append(jnp.concatenate([rows, rows[:lead]], axis=0))
        total = acc[p] + jnp.dot(ws[...], jnp.concatenate(halves, axis=1), preferred_element_type=F32)
        total = jnp.maximum(total + bias, 0.0).astype(BF)
        out_ref[2 * p] = total[:, :w]
        out_ref[2 * p + 1] = total[:, w:]

    for copies in (hcopy, vcopy, qcopy, pcopy, ccopy, kcopy):
        finish(copies)


def place(rows_ref, out_ref):
    out_ref[...] = jnp.swapaxes(rows_ref[...], 0, 1)


def body(nr, nc, current_frame, history_frames, offsets, compress_weight, mixer_weight, mixer_bias):
    frames, ch, h, w = history_frames.shape
    cp = compress_weight.shape[0]
    depth = frames * cp
    reach = h // 2 + 1
    groups = h // 4
    cg = -(-reach // 4)
    mix = mixer_weight.transpose(0, 1, 3, 2)
    anyspace = pl.BlockSpec(memory_space=pl.ANY)
    vmem = pl.BlockSpec(memory_space=pltpu.VMEM)
    joined = pl.pallas_call(
        functools.partial(kernel, nr, nc),
        out_shape=pltpu.VMEM((h, ch, w), BF),
        in_specs=[pl.BlockSpec(memory_space=pltpu.SMEM), anyspace, anyspace, anyspace, vmem, vmem],
        out_specs=vmem,
        scratch_shapes=[
            pltpu.VMEM((frames, ch, h, w), BF),
            pltpu.VMEM((ch, h, w), BF),
            pltpu.VMEM(mix.shape, BF),
            pltpu.VMEM((frames * h, cp, w), BF),
            pltpu.VMEM((frames * h + 4 * reach, cp, w), BF),
            pltpu.VMEM((2, 2 * reach, cp, w), BF),
            pltpu.VMEM((2, 2 * groups, cp, w), BF),
            pltpu.VMEM((4 * groups, cp, w), BF),
            pltpu.VMEM((2, 2 * cg, cp, w), BF),
            pltpu.VMEM((4 * groups + 4 * cg, cp, w), BF),
            pltpu.VMEM((ch, w), BF),
            pltpu.VMEM((2, ch, w), BF),
            pltpu.VMEM((ch, w), BF),
            pltpu.VMEM((2, ch, w), BF),
            pltpu.VMEM(((h + 2) * 3 * ch, w), BF),
            pltpu.VMEM(((h + 2) * 3 * depth, w), BF),
            pltpu.VMEM((h // 2, ch, 2 * w), F32),
            pltpu.VMEM((ch, 9 * ch), BF),
            pltpu.VMEM((ch, -(-9 * depth // 128) * 128), BF),
            pltpu.SemaphoreType.DMA((frames + 2,)),
            pltpu.SemaphoreType.DMA((6, 2)),
            pltpu.SemaphoreType.DMA((6, 2)),
        ],
        compiler_params=pltpu.CompilerParams(collective_id=0, has_side_effects=True),
        name="join",
    )(offsets.T, history_frames, current_frame, mix, compress_weight, mixer_bias)
    return pl.pallas_call(
        place,
        out_shape=jax.ShapeDtypeStruct((ch, h, w), BF),
        in_specs=[vmem],
        out_specs=vmem,
        name="place",
    )(pltpu.with_memory_space_constraint(joined, pltpu.VMEM))


def solution(mesh):
    in_specs = (P(None, "rows", "cols"), P(None, None, "rows", "cols"), P(), P(), P(), P())
    out_specs = P(None, "rows", "cols")
    return jax.shard_map(
        functools.partial(body, mesh.shape["rows"], mesh.shape["cols"]),
        mesh=mesh, in_specs=in_specs, out_specs=out_specs, check_vma=False,
    )
```

```python
import functools

import jax
import jax.numpy as jnp
from jax import lax
from jax.experimental import pallas as pl
from jax.experimental.pallas import tpu as pltpu
from jax.sharding import PartitionSpec as P

MESH = pl.DeviceIdType.MESH
BF = jnp.bfloat16
F32 = jnp.float32
PACK = 7
REACH_X = 17


def pick(ds, positive):
    n = len(ds)
    first, last = jnp.int32(n - 1), jnp.int32(0)
    for k in range(n):
        hit = ds[k] > 0 if positive else ds[k] < 0
        last = jnp.where(hit, jnp.int32(k), last)
    for k in reversed(range(n)):
        hit = ds[k] > 0 if positive else ds[k] < 0
        first = jnp.where(hit, jnp.int32(k), first)
    return first, last


def kernel(
    nr, nc,
    off, hist_hbm, cur_hbm, mix_hbm, cw_ref, bias_ref, out_ref,
    hist, cur, mix, red, vsend, vrecv, hsend, hrecv, csend, crecv,
    qfull, qsend, qrecv, krecv, pk, sp, unp, xs, acc, wp, ws, lsem, ssem, rsem,
):
    frames, ch, h, w = hist.shape
    cp = cw_ref.shape[0]
    depth = frames * cp
    reach = h // 2 + 1
    ring = h + reach
    pitch = w // PACK
    tiles = -(-h // PACK)
    ctiles = -(-reach // PACK)
    pb = 3 * ch
    quarter = ch // 4

    r = lax.axis_index("rows")
    c = lax.axis_index("cols")
    has_up, has_dn, has_lf, has_rt = r > 0, r < nr - 1, c > 0, c < nc - 1
    up_dev, dn_dev, lf_dev, rt_dev = (r - 1, c), (r + 1, c), (r, c - 1), (r, c + 1)

    loads = [pltpu.make_async_copy(hist_hbm.at[k], hist.at[k], lsem.at[k]) for k in range(frames)]
    load_cur = pltpu.make_async_copy(cur_hbm, cur, lsem.at[frames])
    load_mix = pltpu.make_async_copy(mix_hbm, mix, lsem.at[frames + 1])
    for x in (*loads, load_cur, load_mix):
        x.start()

    barrier = pltpu.get_barrier_semaphore()
    for cond, dev in ((has_up, up_dev), (has_dn, dn_dev), (has_lf, lf_dev), (has_rt, rt_dev)):
        @pl.when(cond)
        def _(dev=dev):
            pl.semaphore_signal(barrier, inc=1, device_id=dev, device_id_type=MESH)

    def remote(n, d, src, dst, sideways):
        dev = ((rt_dev, lf_dev) if sideways else (dn_dev, up_dev))[d]
        copy = pltpu.make_async_remote_copy(
            src_ref=src, dst_ref=dst, send_sem=ssem.at[n, d], recv_sem=rsem.at[n, d],
            device_id=dev, device_id_type=MESH,
        )
        ways = (has_rt, has_lf) if sideways else (has_dn, has_up)
        return copy, ways[d], ways[1 - d]

    def start(copies):
        for copy, sends, _ in copies:
            @pl.when(sends)
            def _(copy=copy):
                copy.start()

    def arrive(copies):
        for copy, _, comes in copies:
            @pl.when(comes)
            def _(copy=copy):
                copy.wait_recv()

    def finish(copies):
        for copy, sends, _ in copies:
            @pl.when(sends)
            def _(copy=copy):
                copy.wait_send()

    hcopy = [remote(0, d, hsend.at[d], hrecv.at[d], True) for d in (0, 1)]
    vcopy = [remote(1, d, vsend.at[d], vrecv.at[d], False) for d in (0, 1)]
    qcopy = [remote(2, d, qsend, qrecv.at[d], True) for d in (0, 1)]
    pcopy = [
        remote(3, 0, sp.at[pl.ds(h * pb + ch, ch)], sp.at[pl.ds(ch, ch)], False),
        remote(3, 1, sp.at[pl.ds(pb + ch, ch)], sp.at[pl.ds((h + 1) * pb + ch, ch)], False),
    ]
    ccopy = [remote(4, d, csend.at[d], crecv.at[d], False) for d in (0, 1)]
    kcopy = [remote(5, d, qrecv, krecv.at[d], False) for d in (0, 1)]

    dys = [off[0, k] for k in range(frames)]
    dxs = [off[1, k] for k in range(frames)]
    down, up = pick(dys, True), pick(dys, False)
    right, left = pick(dxs, True), pick(dxs, False)

    def slot(k, d, plus, minus):
        other = jnp.where(d > 0, plus[0], minus[0]) != k
        return jnp.where(other, jnp.int32(1), jnp.int32(0))

    vslot = [slot(k, dys[k], down, up) for k in range(frames)]
    hslot = [slot(k, dxs[k], right, left) for k in range(frames)]
    went_x = [jnp.where(dxs[k] > 0, jnp.int32(0), jnp.int32(1)) for k in range(frames)]
    went_y = [jnp.where(dys[k] > 0, jnp.int32(0), jnp.int32(1)) for k in range(frames)]

    def clear(ref):
        ref[...] = jnp.zeros(ref.shape, BF)

    @pl.when(r == 0)
    def _():
        for ref in (vrecv.at[0], crecv.at[0], krecv.at[0], sp.at[pl.ds(ch, ch)]):
            clear(ref)

    @pl.when(r == nr - 1)
    def _():
        for ref in (vrecv.at[1], crecv.at[1], krecv.at[1], sp.at[pl.ds((h + 1) * pb + ch, ch)]):
            clear(ref)

    @pl.when(c == 0)
    def _():
        clear(hrecv.at[0])
        clear(qrecv.at[0])

    @pl.when(c == nc - 1)
    def _():
        clear(hrecv.at[1])
        clear(qrecv.at[1])

    for k in range(frames):
        loads[k].wait()
        rows = jnp.swapaxes(hist[k], 0, 1)
        for y in range(0, h, 2):
            rhs = jnp.concatenate([rows[y], rows[y + 1]], axis=1)
            got = jnp.dot(cw_ref[...], rhs, preferred_element_type=F32).astype(BF)
            for e in (0, 1):
                red[k * h + y + e] = got[:, e * w:(e + 1) * w]

    lane = lax.broadcasted_iota(jnp.int32, (cp, w), 1)
    for d in (0, 1):
        for s in (0, 1):
            frame, base = (right[s], REACH_X) if d == 0 else (left[s], 0)
            for g in range(tiles):
                tile = None
                for q in range(min(PACK, h - PACK * g)):
                    row = red[frame * h + PACK * g + q]
                    turn = (base + pitch * q) % w
                    row = pltpu.roll(row, turn, 1) if turn else row
                    tile = row if tile is None else jnp.where(lane >= pitch * q, row, tile)
                hsend[d, s * tiles + g] = tile

    count = sum(jnp.where(x, jnp.int32(1), jnp.int32(0)) for x in (has_up, has_dn, has_lf, has_rt))
    pl.semaphore_wait(barrier, count)
    start(hcopy)
    for s in (0, 1):
        vsend[0, pl.ds(s * reach, reach)] = red[pl.ds(down[s] * h + h - reach, reach)]
        vsend[1, pl.ds(s * reach, reach)] = red[pl.ds(up[s] * h, reach)]
    start(vcopy)

    load_cur.wait()
    rows = jnp.swapaxes(cur[...], 0, 1)
    for y in range(h):
        sp[pl.ds((y + 1) * pb + ch, ch)] = rows[y]
    start(pcopy)
    lane_c = lax.broadcasted_iota(jnp.int32, (ch, w), 1)
    tile = jnp.zeros((ch, w), BF)
    for y in range(h):
        turned = pltpu.roll(rows[y], 2 * y + 1, 1)
        tile = jnp.where((lane_c == 2 * y) | (lane_c == 2 * y + 1), turned, tile)
    qfull[...] = tile
    small = qfull[pl.ds(0, quarter)]
    lane_q = lax.broadcasted_iota(jnp.int32, (quarter, w), 1)
    for g in range(1, 4):
        turned = pltpu.roll(qfull[pl.ds(g * quarter, quarter)], 2 * h * g, 1)
        small = jnp.where(lane_q >= 2 * h * g, turned, small)
    qsend[...] = small
    start(qcopy)

    load_mix.wait()
    for i in range(3):
        for j in range(3):
            wp[:, (3 * i + j) * ch:(3 * i + j + 1) * ch] = jnp.swapaxes(mix[i, j, :ch], 0, 1)
    past = [
        mix[i, j, ch + k * cp:ch + (k + 1) * cp] for i in range(3) for k in range(frames) for j in range(3)
    ]
    lead = ws.shape[1] - 9 * depth
    past.append(jnp.zeros((lead, ch), BF))
    past = jnp.concatenate(past, axis=0)
    for n in range(0, ws.shape[1], ch):
        ws[:, n:n + ch] = jnp.swapaxes(past[n:n + ch], 0, 1)
    wide = jnp.broadcast_to(bias_ref[...][None, :], (ch, ch))
    eye = lax.broadcasted_iota(jnp.int32, (ch, ch), 0) == lax.broadcasted_iota(jnp.int32, (ch, ch), 1)
    bias = jnp.sum(jnp.where(eye, wide, 0.0), axis=1, keepdims=True)

    arrive(hcopy)
    for s in (0, 1):
        for d, frame in ((0, down[s]), (1, up[s])):
            way, at = jnp.int32(0), jnp.int32(0)
            for k in range(frames):
                way = jnp.where(frame == k, went_x[k], way)
                at = jnp.where(frame == k, hslot[k] * tiles, at)
            first = at + (tiles - ctiles if d == 0 else 0)
            csend[d, pl.ds(s * ctiles, ctiles)] = hrecv[way, pl.ds(first, ctiles)]
    start(ccopy)
    arrive(qcopy)
    start(kcopy)

    def ends(near, lf_turn, rt_turn):
        lf = jnp.concatenate(
            [pltpu.roll(near[0], (2 * w - 2 * h * g - lf_turn) % w, 1) for g in range(4)], axis=0
        )
        rt = jnp.concatenate(
            [pltpu.roll(near[1], (2 * w - 2 * h * g - rt_turn) % w, 1) for g in range(4)], axis=0
        )
        return jnp.where((lane_c & 1) == 0, lf, rt)

    pk[...] = ends(qrecv, 0, 2)

    masks, kills = [], []
    for k in range(frames):
        plus = dxs[k] > 0
        mine, dead = [], []
        for j in range(3):
            step = dxs[k] + 1 - j
            lo = jnp.where(plus, w - step, 0)
            hi = jnp.where(plus, w, -step)
            mine.append((lane >= lo) & (lane < hi))
            at = jnp.int32(-1)
            if j == 0:
                at = jnp.where(plus | (c > 0), at, -step)
            if j == 2:
                at = jnp.where(plus & (c == nc - 1), w - 1 - step, at)
            dead.append(lane == at)
        masks.append(mine)
        kills.append(dead)

    def unpack(k, m, q, tile):
        turn = (jnp.where(dxs[k] > 0, w - REACH_X, 0) - pitch * q + w) & (w - 1)
        unp[k * ring + m] = pltpu.roll(tile, turn, 1)

    def shift(k, m, row):
        far = unp[k * ring + m]
        for j in range(3):
            near = row if j == 1 else jnp.where(kills[k][j], jnp.zeros_like(row), row)
            both = jnp.where(masks[k][j], far, near)
            xs[(k * ring + m) * 3 + j] = pltpu.roll(both, (dxs[k] + 1 - j + w) & (w - 1), 1)

    for k in range(frames):
        for y in range(h):
            unpack(k, y, y % PACK, hrecv[went_x[k], hslot[k] * tiles + y // PACK])
    for k in range(frames):
        for y in range(h):
            shift(k, y, red[k * h + y])

    def widen(t, edge):
        mid = sp[pl.ds(t * pb + ch, ch)]
        sp[pl.ds(t * pb, ch)] = jnp.where(lane_c == 0, edge, pltpu.roll(mid, 1, 1))
        sp[pl.ds(t * pb + 2 * ch, ch)] = jnp.where(lane_c == w - 1, edge, pltpu.roll(mid, w - 1, 1))

    def present(p):
        y = 2 * p
        rhs = jnp.concatenate([sp[pl.ds(y * pb, 3 * pb)], sp[pl.ds((y + 1) * pb, 3 * pb)]], axis=1)
        acc[p] = jnp.dot(wp[...], rhs, preferred_element_type=F32)

    for t in range(1, h + 1):
        widen(t, pltpu.roll(pk[...], (w - 2 * (t - 1)) % w, 1) if t > 1 else pk[...])
    for p in range(1, h // 2 - 1):
        present(p)
    arrive(pcopy)
    arrive(kcopy)
    widen(0, ends(krecv.at[0], 2 * h - 2, 2 * h))
    widen(h + 1, ends(krecv.at[1], 0, 2))
    present(0)
    present(h // 2 - 1)

    arrive(vcopy)
    arrive(ccopy)
    for k in range(frames):
        for m in range(reach):
            unpack(k, h + m, m % PACK, crecv[went_y[k], vslot[k] * ctiles + m // PACK])
    for k in range(frames):
        for m in range(reach):
            shift(k, h + m, vrecv[went_y[k], vslot[k] * reach + m])

    def window(y):
        rows = []
        for i in range(3):
            for k in range(frames):
                at = y + i - 1 - dys[k]
                at = jnp.where(at < 0, at + ring, at)
                part = xs[pl.ds((k * ring + at) * 3, 3)].reshape(depth, w)
                if y == 0 and i == 0:
                    part = jnp.where(r == 0, jnp.zeros_like(part), part)
                if y == h - 1 and i == 2:
                    part = jnp.where(r == nr - 1, jnp.zeros_like(part), part)
                rows.append(part)
        rows.append(rows[0][:lead])
        return jnp.concatenate(rows, axis=0)

    for p in range(h // 2):
        rhs = jnp.concatenate([window(2 * p), window(2 * p + 1)], axis=1)
        total = acc[p] + jnp.dot(ws[...], rhs, preferred_element_type=F32)
        total = jnp.maximum(total + bias, 0.0).astype(BF)
        out_ref[2 * p] = total[:, :w]
        out_ref[2 * p + 1] = total[:, w:]

    for copies in (hcopy, vcopy, qcopy, pcopy, ccopy, kcopy):
        finish(copies)


def place(rows_ref, out_ref):
    out_ref[...] = jnp.swapaxes(rows_ref[...], 0, 1)


def body(nr, nc, current_frame, history_frames, offsets, compress_weight, mixer_weight, mixer_bias):
    frames, ch, h, w = history_frames.shape
    cp = compress_weight.shape[0]
    depth = frames * cp
    reach = h // 2 + 1
    ring = h + reach
    tiles = -(-h // PACK)
    ctiles = -(-reach // PACK)
    mix = mixer_weight.transpose(0, 1, 3, 2)
    anyspace = pl.BlockSpec(memory_space=pl.ANY)
    vmem = pl.BlockSpec(memory_space=pltpu.VMEM)
    joined = pl.pallas_call(
        functools.partial(kernel, nr, nc),
        out_shape=pltpu.VMEM((h, ch, w), BF),
        in_specs=[pl.BlockSpec(memory_space=pltpu.SMEM), anyspace, anyspace, anyspace, vmem, vmem],
        out_specs=vmem,
        scratch_shapes=[
            pltpu.VMEM((frames, ch, h, w), BF),
            pltpu.VMEM((ch, h, w), BF),
            pltpu.VMEM(mix.shape, BF),
            pltpu.VMEM((frames * h, cp, w), BF),
            pltpu.VMEM((2, 2 * reach, cp, w), BF),
            pltpu.VMEM((2, 2 * reach, cp, w), BF),
            pltpu.VMEM((2, 2 * tiles, cp, w), BF),
            pltpu.VMEM((2, 2 * tiles, cp, w), BF),
            pltpu.VMEM((2, 2 * ctiles, cp, w), BF),
            pltpu.VMEM((2, 2 * ctiles, cp, w), BF),
            pltpu.VMEM((ch, w), BF),
            pltpu.VMEM((ch // 4, w), BF),
            pltpu.VMEM((2, ch // 4, w), BF),
            pltpu.VMEM((2, 2, ch // 4, w), BF),
            pltpu.VMEM((ch, w), BF),
            pltpu.VMEM(((h + 2) * 3 * ch, w), BF),
            pltpu.VMEM((frames * ring, cp, w), BF),
            pltpu.VMEM((frames * ring * 3, cp, w), BF),
            pltpu.VMEM((h // 2, ch, 2 * w), F32),
            pltpu.VMEM((ch, 9 * ch), BF),
            pltpu.VMEM((ch, -(-9 * depth // 128) * 128), BF),
            pltpu.SemaphoreType.DMA((frames + 2,)),
            pltpu.SemaphoreType.DMA((6, 2)),
            pltpu.SemaphoreType.DMA((6, 2)),
        ],
        compiler_params=pltpu.CompilerParams(collective_id=0, has_side_effects=True),
        name="join",
    )(offsets.T, history_frames, current_frame, mix, compress_weight, mixer_bias)
    return pl.pallas_call(
        place,
        out_shape=jax.ShapeDtypeStruct((ch, h, w), BF),
        in_specs=[vmem],
        out_specs=vmem,
        name="place",
    )(pltpu.with_memory_space_constraint(joined, pltpu.VMEM))


def solution(mesh):
    in_specs = (P(None, "rows", "cols"), P(None, None, "rows", "cols"), P(), P(), P(), P())
    out_specs = P(None, "rows", "cols")
    return jax.shard_map(
        functools.partial(body, mesh.shape["rows"], mesh.shape["cols"]),
        mesh=mesh, in_specs=in_specs, out_specs=out_specs, check_vma=False,
    )
```

```python
import functools

import jax
import jax.numpy as jnp
from jax import lax
from jax.experimental import pallas as pl
from jax.experimental.pallas import tpu as pltpu
from jax.sharding import PartitionSpec as P

MESH = pl.DeviceIdType.MESH
BF = jnp.bfloat16
F32 = jnp.float32
PACK = 7
REACH_X = 17


def pick(ds, positive):
    n = len(ds)
    first, last = jnp.int32(n - 1), jnp.int32(0)
    for k in range(n):
        hit = ds[k] > 0 if positive else ds[k] < 0
        last = jnp.where(hit, jnp.int32(k), last)
    for k in reversed(range(n)):
        hit = ds[k] > 0 if positive else ds[k] < 0
        first = jnp.where(hit, jnp.int32(k), first)
    return first, last


def kernel(
    nr, nc,
    off_hbm, hist_hbm, cur_hbm, mix_hbm, cw_hbm, bias_hbm, out_ref,
    off, cw, bias_row, hist, cur, mix, red, vsend, vrecv, packs, hsend, hrecv, csend, crecv,
    qfull, qsend, qrecv, krecv, pk, sp, unp, xs, acc, wp, ws, lsem, ssem, rsem, ready,
):
    frames, ch, h, w = hist.shape
    cp = cw.shape[0]
    depth = frames * cp
    reach = h // 2 + 1
    ring = h + reach
    pitch = w // PACK
    tiles = -(-h // PACK)
    rest = reach - PACK
    pb = 3 * ch
    quarter = ch // 4

    r = lax.axis_index("rows")
    c = lax.axis_index("cols")
    has_up, has_dn, has_lf, has_rt = r > 0, r < nr - 1, c > 0, c < nc - 1
    above, below = (r - 1, has_up), (r + 1, has_dn)
    before, after = (c - 1, has_lf), (c + 1, has_rt)

    small = [
        pltpu.make_async_copy(src, dst, lsem.at[n])
        for n, (src, dst) in enumerate(((off_hbm, off), (cw_hbm, cw), (bias_hbm, bias_row)))
    ]
    loads = [pltpu.make_async_copy(hist_hbm.at[k], hist.at[k], lsem.at[3 + k]) for k in range(frames)]
    load_cur = pltpu.make_async_copy(cur_hbm, cur, lsem.at[3 + frames])
    load_mix = pltpu.make_async_copy(mix_hbm, mix, lsem.at[4 + frames])
    for x in (*loads, *small, load_cur, load_mix):
        x.start()

    barrier = pltpu.get_barrier_semaphore()
    near = ((r - 1, c, has_up), (r + 1, c, has_dn), (r, c - 1, has_lf), (r, c + 1, has_rt))
    for rr, cc, cond in near:
        @pl.when(cond)
        def _(dev=(rr, cc)):
            pl.semaphore_signal(barrier, inc=1, device_id=dev, device_id_type=MESH)

    def number(*conds):
        return sum(jnp.where(x, jnp.int32(1), jnp.int32(0)) for x in conds)

    def remote(n, src, dst, dv=None, dh=None):
        rr, sends, comes, m = r, True, True, 0
        cc = c
        if dv is not None:
            (rr, sends), (_, comes) = (below, above) if dv == 0 else (above, below)
            m = dv
        if dh is not None:
            (cc, out), (_, into) = (after, before) if dh == 0 else (before, after)
            sends, comes = sends & out, comes & into
            m = 2 * m + dh if dv is not None else dh
        copy = pltpu.make_async_remote_copy(
            src_ref=src, dst_ref=dst, send_sem=ssem.at[n, m], recv_sem=rsem.at[n, m],
            device_id=(rr, cc), device_id_type=MESH,
        )
        return copy, sends, comes

    def start(copies):
        for copy, sends, _ in copies:
            @pl.when(sends)
            def _(copy=copy):
                copy.start()

    def arrive(copies):
        for copy, _, comes in copies:
            @pl.when(comes)
            def _(copy=copy):
                copy.wait_recv()

    def finish(copies):
        for copy, sends, _ in copies:
            @pl.when(sends)
            def _(copy=copy):
                copy.wait_send()

    hcopy = [remote(0, hsend.at[d], hrecv.at[d], dh=d) for d in (0, 1)]
    vcopy = [remote(1, vsend.at[d], vrecv.at[d], dv=d) for d in (0, 1)]
    qcopy = [remote(2, qsend, qrecv.at[d], dh=d) for d in (0, 1)]
    pcopy = [
        remote(3, sp.at[pl.ds(h * pb + ch, ch)], sp.at[pl.ds(ch, ch)], dv=0),
        remote(3, sp.at[pl.ds(pb + ch, ch)], sp.at[pl.ds((h + 1) * pb + ch, ch)], dv=1),
    ]
    corners = [(dv, dh) for dv in (0, 1) for dh in (0, 1)]
    ccopy = [remote(4, csend.at[dv], crecv.at[dv, dh], dv, dh) for dv, dh in corners]
    kcopy = [remote(5, qsend, krecv.at[dv, dh], dv, dh) for dv, dh in corners]

    for x in small:
        x.wait()
    dys = [off[0, k] for k in range(frames)]
    dxs = [off[1, k] for k in range(frames)]
    down, up = pick(dys, True), pick(dys, False)
    right, left = pick(dxs, True), pick(dxs, False)

    def slot(k, d, plus, minus):
        other = jnp.where(d > 0, plus[0], minus[0]) != k
        return jnp.where(other, jnp.int32(1), jnp.int32(0))

    vslot = [slot(k, dys[k], down, up) for k in range(frames)]
    hslot = [slot(k, dxs[k], right, left) for k in range(frames)]
    went_x = [jnp.where(dxs[k] > 0, jnp.int32(0), jnp.int32(1)) for k in range(frames)]
    went_y = [jnp.where(dys[k] > 0, jnp.int32(0), jnp.int32(1)) for k in range(frames)]

    def clear(ref):
        ref[...] = jnp.zeros(ref.shape, BF)

    @pl.when(r == 0)
    def _():
        for ref in (vrecv.at[0], crecv.at[0], krecv.at[0], sp.at[pl.ds(ch, ch)]):
            clear(ref)

    @pl.when(r == nr - 1)
    def _():
        for ref in (vrecv.at[1], crecv.at[1], krecv.at[1], sp.at[pl.ds((h + 1) * pb + ch, ch)]):
            clear(ref)

    @pl.when(c == 0)
    def _():
        for ref in (hrecv.at[0], qrecv.at[0], crecv.at[0, 0], crecv.at[1, 0], krecv.at[0, 0], krecv.at[1, 0]):
            clear(ref)

    @pl.when(c == nc - 1)
    def _():
        for ref in (hrecv.at[1], qrecv.at[1], crecv.at[0, 1], crecv.at[1, 1], krecv.at[0, 1], krecv.at[1, 1]):
            clear(ref)

    for k in range(frames):
        loads[k].wait()
        rows = jnp.swapaxes(hist[k], 0, 1)
        for y in range(0, h, 2):
            rhs = jnp.concatenate([rows[y], rows[y + 1]], axis=1)
            got = jnp.dot(cw[...], rhs, preferred_element_type=F32).astype(BF)
            for e in (0, 1):
                red[k * h + y + e] = got[:, e * w:(e + 1) * w]

    for s in (0, 1):
        vsend[0, pl.ds(s * reach, reach)] = red[pl.ds(down[s] * h + h - reach, reach)]
        vsend[1, pl.ds(s * reach, reach)] = red[pl.ds(up[s] * h, reach)]
    pl.semaphore_wait(barrier, number(has_up, has_dn, has_lf, has_rt))
    for rr, cc, cond in near[:2]:
        @pl.when(cond)
        def _(dev=(rr, cc)):
            pl.semaphore_signal(ready, inc=1, device_id=dev, device_id_type=MESH)
    start(vcopy)

    lane = lax.broadcasted_iota(jnp.int32, (cp, w), 1)
    for k in range(frames):
        for g in range(tiles):
            tile = None
            for q in range(min(PACK, h - PACK * g)):
                turn = jnp.where(dxs[k] > 0, jnp.int32((REACH_X + pitch * q) % w), jnp.int32(pitch * q))
                row = pltpu.roll(red[k * h + PACK * g + q], turn, 1)
                tile = row if tile is None else jnp.where(lane >= pitch * q, row, tile)
            packs[k * tiles + g] = tile
    for s in (0, 1):
        for d in (0, 1):
            frame = (right, left)[d][s]
            hsend[d, pl.ds(s * tiles, tiles)] = packs[pl.ds(frame * tiles, tiles)]
    start(hcopy)
    for d in (0, 1):
        at = [(down, up)[d][s] * tiles + (1 if d == 0 else 0) for s in (0, 1)]
        for s in (0, 1):
            csend[d, s] = packs[at[s]]
        turned = pltpu.roll(packs[at[1] + 1], rest * pitch, 1)
        csend[d, 2] = jnp.where(lane < rest * pitch, packs[at[0] + 1], turned)
    pl.semaphore_wait(ready, number(has_up, has_dn))
    start(ccopy)

    load_cur.wait()
    rows = jnp.swapaxes(cur[...], 0, 1)
    for y in range(h):
        sp[pl.ds((y + 1) * pb + ch, ch)] = rows[y]
    lane_c = lax.broadcasted_iota(jnp.int32, (ch, w), 1)
    tile = jnp.zeros((ch, w), BF)
    for y in range(h):
        turned = pltpu.roll(rows[y], 2 * y + 1, 1)
        tile = jnp.where((lane_c == 2 * y) | (lane_c == 2 * y + 1), turned, tile)
    qfull[...] = tile
    small = qfull[pl.ds(0, quarter)]
    lane_q = lax.broadcasted_iota(jnp.int32, (quarter, w), 1)
    for g in range(1, 4):
        turned = pltpu.roll(qfull[pl.ds(g * quarter, quarter)], 2 * h * g, 1)
        small = jnp.where(lane_q >= 2 * h * g, turned, small)
    qsend[...] = small
    start(qcopy)
    start(pcopy)
    start(kcopy)

    load_mix.wait()
    for i in range(3):
        for j in range(3):
            wp[:, (3 * i + j) * ch:(3 * i + j + 1) * ch] = jnp.swapaxes(mix[i, j, :ch], 0, 1)
    past = [
        mix[i, j, ch + k * cp:ch + (k + 1) * cp] for i in range(3) for k in range(frames) for j in range(3)
    ]
    lead = ws.shape[1] - 9 * depth
    past.append(jnp.zeros((lead, ch), BF))
    past = jnp.concatenate(past, axis=0)
    for n in range(0, ws.shape[1], ch):
        ws[:, n:n + ch] = jnp.swapaxes(past[n:n + ch], 0, 1)
    wide = jnp.broadcast_to(bias_row[...][None, :], (ch, ch))
    eye = lax.broadcasted_iota(jnp.int32, (ch, ch), 0) == lax.broadcasted_iota(jnp.int32, (ch, ch), 1)
    bias = jnp.sum(jnp.where(eye, wide, 0.0), axis=1, keepdims=True)

    arrive(hcopy)
    arrive(qcopy)

    def ends(near, lf_turn, rt_turn):
        lf = jnp.concatenate(
            [pltpu.roll(near[0], (2 * w - 2 * h * g - lf_turn) % w, 1) for g in range(4)], axis=0
        )
        rt = jnp.concatenate(
            [pltpu.roll(near[1], (2 * w - 2 * h * g - rt_turn) % w, 1) for g in range(4)], axis=0
        )
        return jnp.where((lane_c & 1) == 0, lf, rt)

    pk[...] = ends(qrecv, 0, 2)

    masks, kills = [], []
    for k in range(frames):
        plus = dxs[k] > 0
        mine, dead = [], []
        for j in range(3):
            step = dxs[k] + 1 - j
            lo = jnp.where(plus, w - step, 0)
            hi = jnp.where(plus, w, -step)
            mine.append((lane >= lo) & (lane < hi))
            at = jnp.int32(-1)
            if j == 0:
                at = jnp.where(plus | (c > 0), at, -step)
            if j == 2:
                at = jnp.where(plus & (c == nc - 1), w - 1 - step, at)
            dead.append(lane == at)
        masks.append(mine)
        kills.append(dead)

    def unpack(k, m, q, tile):
        turn = (jnp.where(dxs[k] > 0, w - REACH_X, 0) - pitch * q + w) & (w - 1)
        unp[k * ring + m] = pltpu.roll(tile, turn, 1)

    def shift(k, m, row):
        far = unp[k * ring + m]
        for j in range(3):
            near = row if j == 1 else jnp.where(kills[k][j], jnp.zeros_like(row), row)
            both = jnp.where(masks[k][j], far, near)
            xs[(k * ring + m) * 3 + j] = pltpu.roll(both, (dxs[k] + 1 - j + w) & (w - 1), 1)

    for k in range(frames):
        for y in range(h):
            unpack(k, y, y % PACK, hrecv[went_x[k], hslot[k] * tiles + y // PACK])
    for k in range(frames):
        for y in range(h):
            shift(k, y, red[k * h + y])

    def widen(t, edge):
        mid = sp[pl.ds(t * pb + ch, ch)]
        sp[pl.ds(t * pb, ch)] = jnp.where(lane_c == 0, edge, pltpu.roll(mid, 1, 1))
        sp[pl.ds(t * pb + 2 * ch, ch)] = jnp.where(lane_c == w - 1, edge, pltpu.roll(mid, w - 1, 1))

    def present(p):
        y = 2 * p
        rhs = jnp.concatenate([sp[pl.ds(y * pb, 3 * pb)], sp[pl.ds((y + 1) * pb, 3 * pb)]], axis=1)
        acc[p] = jnp.dot(wp[...], rhs, preferred_element_type=F32)

    for t in range(1, h + 1):
        widen(t, pltpu.roll(pk[...], (w - 2 * (t - 1)) % w, 1) if t > 1 else pk[...])
    for p in range(1, h // 2 - 1):
        present(p)
    arrive(vcopy)
    arrive(ccopy)
    for k in range(frames):
        for m in range(reach):
            at, q = vslot[k], jnp.int32(m)
            if m >= PACK:
                at, q = 2, rest * vslot[k] + (m - PACK)
            unpack(k, h + m, q, crecv[went_y[k], went_x[k], at])
    for k in range(frames):
        for m in range(reach):
            shift(k, h + m, vrecv[went_y[k], vslot[k] * reach + m])

    def window(y):
        rows = []
        for i in range(3):
            for k in range(frames):
                at = y + i - 1 - dys[k]
                at = jnp.where(at < 0, at + ring, at)
                part = xs[pl.ds((k * ring + at) * 3, 3)].reshape(depth, w)
                if y == 0 and i == 0:
                    part = jnp.where(r == 0, jnp.zeros_like(part), part)
                if y == h - 1 and i == 2:
                    part = jnp.where(r == nr - 1, jnp.zeros_like(part), part)
                rows.append(part)
        rows.append(rows[0][:lead])
        return jnp.concatenate(rows, axis=0)

    def finish_pair(p):
        rhs = jnp.concatenate([window(2 * p), window(2 * p + 1)], axis=1)
        total = acc[p] + jnp.dot(ws[...], rhs, preferred_element_type=F32)
        total = jnp.maximum(total + bias, 0.0).astype(BF)
        out_ref[2 * p] = total[:, :w]
        out_ref[2 * p + 1] = total[:, w:]

    for p in range(1, h // 2 - 1):
        finish_pair(p)
    arrive(pcopy)
    arrive(kcopy)
    widen(0, ends(krecv.at[0], 2 * h - 2, 2 * h))
    widen(h + 1, ends(krecv.at[1], 0, 2))
    for p in (0, h // 2 - 1):
        present(p)
        finish_pair(p)

    for copies in (hcopy, vcopy, qcopy, pcopy, ccopy, kcopy):
        finish(copies)


def place(rows_ref, out_ref):
    out_ref[...] = jnp.swapaxes(rows_ref[...], 0, 1)


def body(nr, nc, current_frame, history_frames, offsets, compress_weight, mixer_weight, mixer_bias):
    frames, ch, h, w = history_frames.shape
    cp = compress_weight.shape[0]
    depth = frames * cp
    reach = h // 2 + 1
    ring = h + reach
    tiles = -(-h // PACK)
    mix = mixer_weight.transpose(0, 1, 3, 2)
    anyspace = pl.BlockSpec(memory_space=pl.ANY)
    vmem = pl.BlockSpec(memory_space=pltpu.VMEM)
    joined = pl.pallas_call(
        functools.partial(kernel, nr, nc),
        out_shape=pltpu.VMEM((h, ch, w), BF),
        in_specs=[anyspace] * 6,
        out_specs=vmem,
        scratch_shapes=[
            pltpu.SMEM((2, frames), jnp.int32),
            pltpu.VMEM((cp, ch), BF),
            pltpu.VMEM((ch,), F32),
            pltpu.VMEM((frames, ch, h, w), BF),
            pltpu.VMEM((ch, h, w), BF),
            pltpu.VMEM(mix.shape, BF),
            pltpu.VMEM((frames * h, cp, w), BF),
            pltpu.VMEM((2, 2 * reach, cp, w), BF),
            pltpu.VMEM((2, 2 * reach, cp, w), BF),
            pltpu.VMEM((frames * tiles, cp, w), BF),
            pltpu.VMEM((2, 2 * tiles, cp, w), BF),
            pltpu.VMEM((2, 2 * tiles, cp, w), BF),
            pltpu.VMEM((2, 3, cp, w), BF),
            pltpu.VMEM((2, 2, 3, cp, w), BF),
            pltpu.VMEM((ch, w), BF),
            pltpu.VMEM((ch // 4, w), BF),
            pltpu.VMEM((2, ch // 4, w), BF),
            pltpu.VMEM((2, 2, ch // 4, w), BF),
            pltpu.VMEM((ch, w), BF),
            pltpu.VMEM(((h + 2) * 3 * ch, w), BF),
            pltpu.VMEM((frames * ring, cp, w), BF),
            pltpu.VMEM((frames * ring * 3, cp, w), BF),
            pltpu.VMEM((h // 2, ch, 2 * w), F32),
            pltpu.VMEM((ch, 9 * ch), BF),
            pltpu.VMEM((ch, -(-9 * depth // 128) * 128), BF),
            pltpu.SemaphoreType.DMA((frames + 5,)),
            pltpu.SemaphoreType.DMA((6, 4)),
            pltpu.SemaphoreType.DMA((6, 4)),
            pltpu.SemaphoreType.REGULAR,
        ],
        compiler_params=pltpu.CompilerParams(collective_id=0, has_side_effects=True),
        name="join",
    )(offsets.T, history_frames, current_frame, mix, compress_weight, mixer_bias)
    return pl.pallas_call(
        place,
        out_shape=jax.ShapeDtypeStruct((ch, h, w), BF),
        in_specs=[vmem],
        out_specs=vmem,
        name="place",
    )(pltpu.with_memory_space_constraint(joined, pltpu.VMEM))


def solution(mesh):
    in_specs = (P(None, "rows", "cols"), P(None, None, "rows", "cols"), P(), P(), P(), P())
    out_specs = P(None, "rows", "cols")
    return jax.shard_map(
        functools.partial(body, mesh.shape["rows"], mesh.shape["cols"]),
        mesh=mesh, in_specs=in_specs, out_specs=out_specs, check_vma=False,
    )
```

```python
import functools

import jax
import jax.numpy as jnp
from jax import lax
from jax.experimental import pallas as pl
from jax.experimental.pallas import tpu as pltpu
from jax.sharding import PartitionSpec as P

MESH = pl.DeviceIdType.MESH
BF = jnp.bfloat16
F32 = jnp.float32
PACK = 7
CHUNKS = 4
REACH_X = 17


def pick(ds, positive):
    n = len(ds)
    first, last = jnp.int32(n - 1), jnp.int32(0)
    for k in range(n):
        hit = ds[k] > 0 if positive else ds[k] < 0
        last = jnp.where(hit, jnp.int32(k), last)
    for k in reversed(range(n)):
        hit = ds[k] > 0 if positive else ds[k] < 0
        first = jnp.where(hit, jnp.int32(k), first)
    return first, last


def kernel(
    nr, nc,
    off_hbm, hist_hbm, cur_hbm, mix_hbm, cw_hbm, bias_hbm, out_ref,
    off, cw, bias_row, hist, cur, mix, red, vsend, vrecv, packs, hsend, hrecv, csend, crecv_a, crecv_b,
    qfull, qsend, qrecv, krecv, pk, sp, unp, xs, acc, wp, ws, lsem, ssem, rsem, ready,
):
    frames, ch, h, w = hist.shape
    cp = cw.shape[0]
    depth = frames * cp
    reach = h // 2 + 1
    pitch = w // PACK
    tiles = -(-h // PACK)
    rest = reach - PACK
    own = frames * h
    pb = 3 * ch
    quarter = ch // 4

    r = lax.axis_index("rows")
    c = lax.axis_index("cols")
    has_up, has_dn, has_lf, has_rt = r > 0, r < nr - 1, c > 0, c < nc - 1
    above, below = (r - 1, has_up), (r + 1, has_dn)
    before, after = (c - 1, has_lf), (c + 1, has_rt)

    barrier = pltpu.get_barrier_semaphore()
    near = ((r - 1, c, has_up), (r + 1, c, has_dn), (r, c - 1, has_lf), (r, c + 1, has_rt))
    for rr, cc, cond in near:
        @pl.when(cond)
        def _(dev=(rr, cc)):
            pl.semaphore_signal(barrier, inc=1, device_id=dev, device_id_type=MESH)

    small = [
        pltpu.make_async_copy(src, dst, lsem.at[n])
        for n, (src, dst) in enumerate(((off_hbm, off), (cw_hbm, cw), (bias_hbm, bias_row)))
    ]
    loads = [pltpu.make_async_copy(hist_hbm.at[k], hist.at[k], lsem.at[3 + k]) for k in range(frames)]
    load_cur = pltpu.make_async_copy(cur_hbm, cur, lsem.at[3 + frames])
    load_mix = pltpu.make_async_copy(mix_hbm, mix, lsem.at[4 + frames])
    for x in (load_cur, *loads, *small, load_mix):
        x.start()

    def number(*conds):
        return sum(jnp.where(x, jnp.int32(1), jnp.int32(0)) for x in conds)

    def remote(n, src, dst, dv=None, dh=None):
        rr, sends, comes, m = r, True, True, 0
        cc = c
        if dv is not None:
            (rr, sends), (_, comes) = (below, above) if dv == 0 else (above, below)
            m = dv
        if dh is not None:
            (cc, out), (_, into) = (after, before) if dh == 0 else (before, after)
            sends, comes = sends & out, comes & into
            m = 2 * m + dh if dv is not None else dh
        copy = pltpu.make_async_remote_copy(
            src_ref=src, dst_ref=dst, send_sem=ssem.at[n, m], recv_sem=rsem.at[n, m],
            device_id=(rr, cc), device_id_type=MESH,
        )
        return copy, sends, comes

    def start(copies):
        for copy, sends, _ in copies:
            @pl.when(sends)
            def _(copy=copy):
                copy.start()

    def arrive(copies):
        for copy, _, comes in copies:
            @pl.when(comes)
            def _(copy=copy):
                copy.wait_recv()

    def finish(copies):
        for copy, sends, _ in copies:
            @pl.when(sends)
            def _(copy=copy):
                copy.wait_send()

    hcopy = [remote(0, hsend.at[d], hrecv.at[d], dh=d) for d in (0, 1)]
    def vpart(n, s):
        part = pl.ds(s * reach, reach)
        return [remote(n, vsend.at[d, part], vrecv.at[d, part], dv=d) for d in (0, 1)]

    vcopy, wcopy = vpart(1, 0), vpart(6, 1)
    qcopy = [remote(2, qsend, qrecv.at[d], dh=d) for d in (0, 1)]
    pcopy = [
        remote(3, sp.at[pl.ds(h * pb + ch, ch)], sp.at[pl.ds(ch, ch)], dv=0),
        remote(3, sp.at[pl.ds(pb + ch, ch)], sp.at[pl.ds((h + 1) * pb + ch, ch)], dv=1),
    ]
    crecv = (crecv_a, crecv_b)
    corners = [(dv, dh) for dv in (0, 1) for dh in (0, 1)]
    ccopy = [remote(4, csend.at[dv], crecv[dv].at[dh], dv, dh) for dv, dh in corners]
    kcopy = [remote(5, qsend, krecv.at[dv, dh], dv, dh) for dv, dh in corners]

    def clear(ref):
        ref[...] = jnp.zeros(ref.shape, BF)

    @pl.when(r == 0)
    def _():
        for ref in (xs.at[pl.ds(own * 3, 6 * reach)], krecv.at[0], sp.at[pl.ds(ch, ch)]):
            clear(ref)

    @pl.when(r == nr - 1)
    def _():
        for ref in (xs.at[pl.ds((own + 2 * reach) * 3, 6 * reach)], krecv.at[1], sp.at[pl.ds((h + 1) * pb + ch, ch)]):
            clear(ref)

    @pl.when(c == 0)
    def _():
        for ref in (hrecv.at[0], qrecv.at[0], crecv[0].at[0], crecv[1].at[0], krecv.at[0, 0], krecv.at[1, 0]):
            clear(ref)

    @pl.when(c == nc - 1)
    def _():
        for ref in (hrecv.at[1], qrecv.at[1], crecv[0].at[1], crecv[1].at[1], krecv.at[0, 1], krecv.at[1, 1]):
            clear(ref)

    for x in small:
        x.wait()
    dys = [off[0, k] for k in range(frames)]
    dxs = [off[1, k] for k in range(frames)]
    down, up = pick(dys, True), pick(dys, False)
    right, left = pick(dxs, True), pick(dxs, False)

    def slot(k, d, plus, minus):
        other = jnp.where(d > 0, plus[0], minus[0]) != k
        return jnp.where(other, jnp.int32(1), jnp.int32(0))

    vslot = [slot(k, dys[k], down, up) for k in range(frames)]
    hslot = [slot(k, dxs[k], right, left) for k in range(frames)]
    went_x = [jnp.where(dxs[k] > 0, jnp.int32(0), jnp.int32(1)) for k in range(frames)]
    went_y = [jnp.where(dys[k] > 0, jnp.int32(0), jnp.int32(1)) for k in range(frames)]

    load_cur.wait()
    rows = jnp.swapaxes(cur[...], 0, 1)
    for y in range(h):
        sp[pl.ds((y + 1) * pb + ch, ch)] = rows[y]
    lane_c = lax.broadcasted_iota(jnp.int32, (ch, w), 1)
    tile = jnp.zeros((ch, w), BF)
    for y in range(h):
        turned = pltpu.roll(rows[y], 2 * y + 1, 1)
        tile = jnp.where((lane_c == 2 * y) | (lane_c == 2 * y + 1), turned, tile)
    qfull[...] = tile
    small = qfull[pl.ds(0, quarter)]
    lane_q = lax.broadcasted_iota(jnp.int32, (quarter, w), 1)
    for g in range(1, 4):
        turned = pltpu.roll(qfull[pl.ds(g * quarter, quarter)], 2 * h * g, 1)
        small = jnp.where(lane_q >= 2 * h * g, turned, small)
    qsend[...] = small

    for k in range(frames):
        if k == 2:
            pl.semaphore_wait(barrier, number(has_up, has_dn, has_lf, has_rt))
            for rr, cc, cond in near[:2]:
                @pl.when(cond)
                def _(dev=(rr, cc)):
                    pl.semaphore_signal(ready, inc=1, device_id=dev, device_id_type=MESH)
            start(qcopy)
            start(pcopy)
        loads[k].wait()
        rows = jnp.swapaxes(hist[k], 0, 1)
        for y in range(0, h, 2):
            rhs = jnp.concatenate([rows[y], rows[y + 1]], axis=1)
            got = jnp.dot(cw[...], rhs, preferred_element_type=F32).astype(BF)
            for e in (0, 1):
                red[k * h + y + e] = got[:, e * w:(e + 1) * w]

    lane = lax.broadcasted_iota(jnp.int32, (cp, w), 1)
    for k in range(frames):
        for g in range(tiles):
            tile = None
            for q in range(min(PACK, h - PACK * g)):
                turn = jnp.where(dxs[k] > 0, jnp.int32((REACH_X + pitch * q) % w), jnp.int32(pitch * q))
                row = pltpu.roll(red[k * h + PACK * g + q], turn, 1)
                tile = row if tile is None else jnp.where(lane >= pitch * q, row, tile)
            packs[k * tiles + g] = tile
    for s in (0, 1):
        for d in (0, 1):
            frame = (right, left)[d][s]
            hsend[d, pl.ds(s * tiles, tiles)] = packs[pl.ds(frame * tiles, tiles)]
    start(hcopy)
    for s in (0, 1):
        vsend[0, pl.ds(s * reach, reach)] = red[pl.ds(down[s] * h + h - reach, reach)]
        vsend[1, pl.ds(s * reach, reach)] = red[pl.ds(up[s] * h, reach)]
    start(vcopy)

    for d in (0, 1):
        at = [(down, up)[d][s] * tiles + (1 if d == 0 else 0) for s in (0, 1)]
        for s in (0, 1):
            csend[d, s] = packs[at[s]]
        turned = pltpu.roll(packs[at[1] + 1], rest * pitch, 1)
        csend[d, 2] = jnp.where(lane < rest * pitch, packs[at[0] + 1], turned)
    pl.semaphore_wait(ready, number(has_up, has_dn))
    start(ccopy)
    start(kcopy)
    start(wcopy)

    load_mix.wait()
    for i in range(3):
        for j in range(3):
            wp[:, (3 * i + j) * ch:(3 * i + j + 1) * ch] = jnp.swapaxes(mix[i, j, :ch], 0, 1)
    past = [
        mix[i, j, ch + k * cp:ch + (k + 1) * cp] for i in range(3) for k in range(frames) for j in range(3)
    ]
    lead = ws.shape[1] - 9 * depth
    past.append(jnp.zeros((lead, ch), BF))
    past = jnp.concatenate(past, axis=0)
    for n in range(0, ws.shape[1], ch):
        ws[:, n:n + ch] = jnp.swapaxes(past[n:n + ch], 0, 1)
    wide = jnp.broadcast_to(bias_row[...][None, :], (ch, ch))
    eye = lax.broadcasted_iota(jnp.int32, (ch, ch), 0) == lax.broadcasted_iota(jnp.int32, (ch, ch), 1)
    bias = jnp.sum(jnp.where(eye, wide, 0.0), axis=1, keepdims=True)

    arrive(qcopy)

    def ends(near, lf_turn, rt_turn):
        lf = jnp.concatenate(
            [pltpu.roll(near[0], (2 * w - 2 * h * g - lf_turn) % w, 1) for g in range(4)], axis=0
        )
        rt = jnp.concatenate(
            [pltpu.roll(near[1], (2 * w - 2 * h * g - rt_turn) % w, 1) for g in range(4)], axis=0
        )
        return jnp.where((lane_c & 1) == 0, lf, rt)

    pk[...] = ends(qrecv, 0, 2)

    def shifter(dx):
        plus = dx > 0
        masks, kills = [], []
        for j in range(3):
            step = dx + 1 - j
            lo = jnp.where(plus, w - step, 0)
            hi = jnp.where(plus, w, -step)
            masks.append((lane >= lo) & (lane < hi))
            at = jnp.int32(-1)
            if j == 0:
                at = jnp.where(plus | (c > 0), at, -step)
            if j == 2:
                at = jnp.where(plus & (c == nc - 1), w - 1 - step, at)
            kills.append(lane == at)

        def unpack(at, q, tile):
            turn = (jnp.where(plus, w - REACH_X, 0) - pitch * q + w) & (w - 1)
            unp[at] = pltpu.roll(tile, turn, 1)

        def shift(at, row):
            far = unp[at]
            for j in range(3):
                near = row if j == 1 else jnp.where(kills[j], jnp.zeros_like(row), row)
                both = jnp.where(masks[j], far, near)
                xs[at * 3 + j] = pltpu.roll(both, (dx + 1 - j + w) & (w - 1), 1)

        return unpack, shift

    def halo(d):
        arrive([vcopy[d], wcopy[d], ccopy[2 * d], ccopy[2 * d + 1]])
        @pl.when((has_up, has_dn)[d])
        def _():
            for s in (0, 1):
                dx = off[1, (down, up)[d][s]]
                side = jnp.where(dx > 0, jnp.int32(0), jnp.int32(1))
                unpack, shift = shifter(dx)
                first = own + (2 * d + s) * reach
                for m in range(reach):
                    if m < PACK:
                        unpack(first + m, m, crecv[d][side, s])
                    else:
                        unpack(first + m, rest * s + m - PACK, crecv[d][side, 2])
                for m in range(reach):
                    shift(first + m, vrecv[d, s * reach + m])

    def widen(t, edge):
        mid = sp[pl.ds(t * pb + ch, ch)]
        sp[pl.ds(t * pb, ch)] = jnp.where(lane_c == 0, edge, pltpu.roll(mid, 1, 1))
        sp[pl.ds(t * pb + 2 * ch, ch)] = jnp.where(lane_c == w - 1, edge, pltpu.roll(mid, w - 1, 1))

    def present(p):
        y = 2 * p
        rhs = jnp.concatenate([sp[pl.ds(y * pb, 3 * pb)], sp[pl.ds((y + 1) * pb, 3 * pb)]], axis=1)
        acc[p] = jnp.dot(wp[...], rhs, preferred_element_type=F32)

    for t in range(1, h + 1):
        widen(t, pltpu.roll(pk[...], (w - 2 * (t - 1)) % w, 1) if t > 1 else pk[...])
    for p in range(1, h // 2 - 1):
        present(p)
    arrive(hcopy)
    for k in range(frames):
        unpack, shift = shifter(dxs[k])
        for y in range(h):
            unpack(k * h + y, y % PACK, hrecv[went_x[k], hslot[k] * tiles + y // PACK])
        for y in range(h):
            shift(k * h + y, red[k * h + y])

    def window(y):
        rows = []
        for i in range(3):
            for k in range(frames):
                at = y + i - 1 - dys[k]
                at = jnp.where(
                    at < 0, own + vslot[k] * reach + reach + at,
                    jnp.where(at >= h, own + (2 + vslot[k]) * reach + at - h, k * h + at),
                )
                part = xs[pl.ds(at * 3, 3)].reshape(depth, w)
                if y == 0 and i == 0:
                    part = jnp.where(r == 0, jnp.zeros_like(part), part)
                if y == h - 1 and i == 2:
                    part = jnp.where(r == nr - 1, jnp.zeros_like(part), part)
                rows.append(part)
        rows.append(rows[0][:lead])
        return jnp.concatenate(rows, axis=0)

    def finish_pair(p):
        rhs = jnp.concatenate([window(2 * p), window(2 * p + 1)], axis=1)
        total = acc[p] + jnp.dot(ws[...], rhs, preferred_element_type=F32)
        total = jnp.maximum(total + bias, 0.0).astype(BF)
        out_ref[2 * p] = total[:, :w]
        out_ref[2 * p + 1] = total[:, w:]

    last = h // 2 - 1
    free = (h - reach - 1) // 2

    def edge_pair(d):
        arrive([pcopy[d], kcopy[2 * d], kcopy[2 * d + 1]])
        if d == 0:
            widen(0, ends(krecv.at[0], 2 * h - 2, 2 * h))
        else:
            widen(h + 1, ends(krecv.at[1], 0, 2))
        present(last * d)
        finish_pair(last * d)

    first_above = (r % 2 == 1) | (r == 0)

    @pl.when(first_above)
    def _():
        halo(0)
        for p in range(1, free):
            finish_pair(p)
        edge_pair(0)
        halo(1)
        for p in range(free, last):
            finish_pair(p)
        edge_pair(1)

    @pl.when(jnp.logical_not(first_above))
    def _():
        halo(1)
        for p in range(last + 1 - free, last):
            finish_pair(p)
        edge_pair(1)
        halo(0)
        for p in range(1, last + 1 - free):
            finish_pair(p)
        edge_pair(0)

    for copies in (hcopy, vcopy, wcopy, qcopy, pcopy, ccopy, kcopy):
        finish(copies)


def place(rows_ref, out_hbm, turned, sem):
    n = out_hbm.shape[0] // CHUNKS
    copies = []
    for g in range(CHUNKS):
        part = pl.ds(g * n, n)
        turned[part] = jnp.swapaxes(rows_ref[:, part], 0, 1)
        copies.append(pltpu.make_async_copy(turned.at[part], out_hbm.at[part], sem.at[g]))
        copies[-1].start()
    for copy in copies:
        copy.wait()


def body(nr, nc, current_frame, history_frames, offsets, compress_weight, mixer_weight, mixer_bias):
    frames, ch, h, w = history_frames.shape
    cp = compress_weight.shape[0]
    depth = frames * cp
    reach = h // 2 + 1
    rows = frames * h + 4 * reach
    tiles = -(-h // PACK)
    mix = mixer_weight.transpose(0, 1, 3, 2)
    anyspace = pl.BlockSpec(memory_space=pl.ANY)
    vmem = pl.BlockSpec(memory_space=pltpu.VMEM)
    joined = pl.pallas_call(
        functools.partial(kernel, nr, nc),
        out_shape=pltpu.VMEM((h, ch, w), BF),
        in_specs=[anyspace] * 6,
        out_specs=vmem,
        scratch_shapes=[
            pltpu.SMEM((2, frames), jnp.int32),
            pltpu.VMEM((cp, ch), BF),
            pltpu.VMEM((ch,), F32),
            pltpu.VMEM((frames, ch, h, w), BF),
            pltpu.VMEM((ch, h, w), BF),
            pltpu.VMEM(mix.shape, BF),
            pltpu.VMEM((frames * h, cp, w), BF),
            pltpu.VMEM((2, 2 * reach, cp, w), BF),
            pltpu.VMEM((2, 2 * reach, cp, w), BF),
            pltpu.VMEM((frames * tiles, cp, w), BF),
            pltpu.VMEM((2, 2 * tiles, cp, w), BF),
            pltpu.VMEM((2, 2 * tiles, cp, w), BF),
            pltpu.VMEM((2, 3, cp, w), BF),
            pltpu.VMEM((2, 3, cp, w), BF),
            pltpu.VMEM((2, 3, cp, w), BF),
            pltpu.VMEM((ch, w), BF),
            pltpu.VMEM((ch // 4, w), BF),
            pltpu.VMEM((2, ch // 4, w), BF),
            pltpu.VMEM((2, 2, ch // 4, w), BF),
            pltpu.VMEM((ch, w), BF),
            pltpu.VMEM(((h + 2) * 3 * ch, w), BF),
            pltpu.VMEM((rows, cp, w), BF),
            pltpu.VMEM((rows * 3, cp, w), BF),
            pltpu.VMEM((h // 2, ch, 2 * w), F32),
            pltpu.VMEM((ch, 9 * ch), BF),
            pltpu.VMEM((ch, -(-9 * depth // 128) * 128), BF),
            pltpu.SemaphoreType.DMA((frames + 5,)),
            pltpu.SemaphoreType.DMA((7, 4)),
            pltpu.SemaphoreType.DMA((7, 4)),
            pltpu.SemaphoreType.REGULAR,
        ],
        compiler_params=pltpu.CompilerParams(collective_id=0, has_side_effects=True),
        name="join",
    )(offsets.T, history_frames, current_frame, mix, compress_weight, mixer_bias)
    return pl.pallas_call(
        place,
        out_shape=jax.ShapeDtypeStruct((ch, h, w), BF),
        in_specs=[vmem],
        out_specs=anyspace,
        scratch_shapes=[pltpu.VMEM((ch, h, w), BF), pltpu.SemaphoreType.DMA((CHUNKS,))],
        name="place",
    )(pltpu.with_memory_space_constraint(joined, pltpu.VMEM))


def solution(mesh):
    in_specs = (P(None, "rows", "cols"), P(None, None, "rows", "cols"), P(), P(), P(), P())
    out_specs = P(None, "rows", "cols")
    return jax.shard_map(
        functools.partial(body, mesh.shape["rows"], mesh.shape["cols"]),
        mesh=mesh, in_specs=in_specs, out_specs=out_specs, check_vma=False,
    )
```

```python
import functools

import jax
import jax.numpy as jnp
from jax import lax
from jax.experimental import pallas as pl
from jax.experimental.pallas import tpu as pltpu
from jax.sharding import PartitionSpec as P

MESH = pl.DeviceIdType.MESH
BF = jnp.bfloat16
F32 = jnp.float32
PACK = 7
CHUNKS = 4
REACH_X = 17


def pick(ds, positive):
    n = len(ds)
    first, last = jnp.int32(n - 1), jnp.int32(0)
    for k in range(n):
        hit = ds[k] > 0 if positive else ds[k] < 0
        last = jnp.where(hit, jnp.int32(k), last)
    for k in reversed(range(n)):
        hit = ds[k] > 0 if positive else ds[k] < 0
        first = jnp.where(hit, jnp.int32(k), first)
    return first, last


def kernel(
    nr, nc,
    off_hbm, hist_hbm, cur_hbm, mix_hbm, cw_hbm, bias_hbm, out_ref,
    off, cw, bias_row, hist, cur, mix, red, vsend, vrecv, packs, hsend, hrecv, csend, crecv_a, crecv_b,
    qfull, qsend, qrecv, krecv, pk, sp, unp, xs, acc, wp, ws, lsem, ssem, rsem, ready,
):
    frames, ch, h, w = hist.shape
    cp = cw.shape[0]
    depth = frames * cp
    reach = h // 2 + 1
    pitch = w // PACK
    tiles = -(-h // PACK)
    rest = reach - PACK
    own = frames * h
    pb = 3 * ch
    quarter = ch // 4

    r = lax.axis_index("rows")
    c = lax.axis_index("cols")
    has_up, has_dn, has_lf, has_rt = r > 0, r < nr - 1, c > 0, c < nc - 1
    above, below = (r - 1, has_up), (r + 1, has_dn)
    before, after = (c - 1, has_lf), (c + 1, has_rt)

    barrier = pltpu.get_barrier_semaphore()
    near = ((r - 1, c, has_up), (r + 1, c, has_dn), (r, c - 1, has_lf), (r, c + 1, has_rt))
    for rr, cc, cond in near:
        @pl.when(cond)
        def _(dev=(rr, cc)):
            pl.semaphore_signal(barrier, inc=1, device_id=dev, device_id_type=MESH)

    small = [
        pltpu.make_async_copy(src, dst, lsem.at[n])
        for n, (src, dst) in enumerate(((off_hbm, off), (cw_hbm, cw), (bias_hbm, bias_row)))
    ]
    loads = [pltpu.make_async_copy(hist_hbm.at[k], hist.at[k], lsem.at[3 + k]) for k in range(frames)]
    load_cur = pltpu.make_async_copy(cur_hbm, cur, lsem.at[3 + frames])
    load_mix = pltpu.make_async_copy(mix_hbm, mix, lsem.at[4 + frames])
    for x in (load_cur, *loads, *small, load_mix):
        x.start()

    def number(*conds):
        return sum(jnp.where(x, jnp.int32(1), jnp.int32(0)) for x in conds)

    def remote(n, src, dst, dv=None, dh=None):
        rr, sends, comes, m = r, True, True, 0
        cc = c
        if dv is not None:
            (rr, sends), (_, comes) = (below, above) if dv == 0 else (above, below)
            m = dv
        if dh is not None:
            (cc, out), (_, into) = (after, before) if dh == 0 else (before, after)
            sends, comes = sends & out, comes & into
            m = 2 * m + dh if dv is not None else dh
        copy = pltpu.make_async_remote_copy(
            src_ref=src, dst_ref=dst, send_sem=ssem.at[n, m], recv_sem=rsem.at[n, m],
            device_id=(rr, cc), device_id_type=MESH,
        )
        return copy, sends, comes

    def start(copies):
        for copy, sends, _ in copies:
            @pl.when(sends)
            def _(copy=copy):
                copy.start()

    def arrive(copies):
        for copy, _, comes in copies:
            @pl.when(comes)
            def _(copy=copy):
                copy.wait_recv()

    def finish(copies):
        for copy, sends, _ in copies:
            @pl.when(sends)
            def _(copy=copy):
                copy.wait_send()

    hcopy = [remote(0, hsend.at[d], hrecv.at[d], dh=d) for d in (0, 1)]
    def vpart(n, s):
        part = pl.ds(s * reach, reach)
        return [remote(n, vsend.at[d, part], vrecv.at[d, part], dv=d) for d in (0, 1)]

    vcopy, wcopy = vpart(1, 0), vpart(6, 1)
    qcopy = [remote(2, qsend, qrecv.at[d], dh=d) for d in (0, 1)]
    pcopy = [
        remote(3, sp.at[pl.ds(h * pb + ch, ch)], sp.at[pl.ds(ch, ch)], dv=0),
        remote(3, sp.at[pl.ds(pb + ch, ch)], sp.at[pl.ds((h + 1) * pb + ch, ch)], dv=1),
    ]
    crecv = (crecv_a, crecv_b)
    corners = [(dv, dh) for dv in (0, 1) for dh in (0, 1)]
    ccopy = [remote(4, csend.at[dv], crecv[dv].at[dh], dv, dh) for dv, dh in corners]
    kcopy = [remote(5, qsend, krecv.at[dv, dh], dv, dh) for dv, dh in corners]

    def clear(ref):
        ref[...] = jnp.zeros(ref.shape, BF)

    @pl.when(r == 0)
    def _():
        for ref in (xs.at[pl.ds(own * 3, 6 * reach)], krecv.at[0], sp.at[pl.ds(ch, ch)]):
            clear(ref)

    @pl.when(r == nr - 1)
    def _():
        for ref in (xs.at[pl.ds((own + 2 * reach) * 3, 6 * reach)], krecv.at[1], sp.at[pl.ds((h + 1) * pb + ch, ch)]):
            clear(ref)

    @pl.when(c == 0)
    def _():
        for ref in (hrecv.at[0], qrecv.at[0], crecv[0].at[0], crecv[1].at[0], krecv.at[0, 0], krecv.at[1, 0]):
            clear(ref)

    @pl.when(c == nc - 1)
    def _():
        for ref in (hrecv.at[1], qrecv.at[1], crecv[0].at[1], crecv[1].at[1], krecv.at[0, 1], krecv.at[1, 1]):
            clear(ref)

    for x in small:
        x.wait()
    dys = [off[0, k] for k in range(frames)]
    dxs = [off[1, k] for k in range(frames)]
    down, up = pick(dys, True), pick(dys, False)
    right, left = pick(dxs, True), pick(dxs, False)

    def slot(k, d, plus, minus):
        other = jnp.where(d > 0, plus[0], minus[0]) != k
        return jnp.where(other, jnp.int32(1), jnp.int32(0))

    vslot = [slot(k, dys[k], down, up) for k in range(frames)]
    hslot = [slot(k, dxs[k], right, left) for k in range(frames)]
    went_x = [jnp.where(dxs[k] > 0, jnp.int32(0), jnp.int32(1)) for k in range(frames)]
    went_y = [jnp.where(dys[k] > 0, jnp.int32(0), jnp.int32(1)) for k in range(frames)]

    load_cur.wait()
    rows = jnp.swapaxes(cur[...], 0, 1)
    for y in range(h):
        sp[pl.ds((y + 1) * pb + ch, ch)] = rows[y]
    lane_c = lax.broadcasted_iota(jnp.int32, (ch, w), 1)
    tile = jnp.zeros((ch, w), BF)
    for y in range(h):
        turned = pltpu.roll(rows[y], 2 * y + 1, 1)
        tile = jnp.where((lane_c == 2 * y) | (lane_c == 2 * y + 1), turned, tile)
    qfull[...] = tile
    small = qfull[pl.ds(0, quarter)]
    lane_q = lax.broadcasted_iota(jnp.int32, (quarter, w), 1)
    for g in range(1, 4):
        turned = pltpu.roll(qfull[pl.ds(g * quarter, quarter)], 2 * h * g, 1)
        small = jnp.where(lane_q >= 2 * h * g, turned, small)
    qsend[...] = small

    for k in range(frames):
        if k == 2:
            pl.semaphore_wait(barrier, number(has_up, has_dn, has_lf, has_rt))
            for rr, cc, cond in near[:2]:
                @pl.when(cond)
                def _(dev=(rr, cc)):
                    pl.semaphore_signal(ready, inc=1, device_id=dev, device_id_type=MESH)
            start(qcopy)
            start(pcopy)
        loads[k].wait()
        rows = jnp.swapaxes(hist[k], 0, 1)
        for y in range(0, h, 2):
            rhs = jnp.concatenate([rows[y], rows[y + 1]], axis=1)
            got = jnp.dot(cw[...], rhs, preferred_element_type=F32).astype(BF)
            for e in (0, 1):
                red[k * h + y + e] = got[:, e * w:(e + 1) * w]

    lane = lax.broadcasted_iota(jnp.int32, (cp, w), 1)
    for k in range(frames):
        for g in range(tiles):
            tile = None
            for q in range(min(PACK, h - PACK * g)):
                turn = jnp.where(dxs[k] > 0, jnp.int32((REACH_X + pitch * q) % w), jnp.int32(pitch * q))
                row = pltpu.roll(red[k * h + PACK * g + q], turn, 1)
                tile = row if tile is None else jnp.where(lane >= pitch * q, row, tile)
            packs[k * tiles + g] = tile
    for s in (0, 1):
        for d in (0, 1):
            frame = (right, left)[d][s]
            hsend[d, pl.ds(s * tiles, tiles)] = packs[pl.ds(frame * tiles, tiles)]
    start(hcopy)
    for s in (0, 1):
        vsend[0, pl.ds(s * reach, reach)] = red[pl.ds(down[s] * h + h - reach, reach)]
        vsend[1, pl.ds(s * reach, reach)] = red[pl.ds(up[s] * h, reach)]
    start(vcopy)

    for d in (0, 1):
        at = [(down, up)[d][s] * tiles + (1 if d == 0 else 0) for s in (0, 1)]
        for s in (0, 1):
            csend[d, s] = packs[at[s]]
        turned = pltpu.roll(packs[at[1] + 1], rest * pitch, 1)
        csend[d, 2] = jnp.where(lane < rest * pitch, packs[at[0] + 1], turned)
    pl.semaphore_wait(ready, number(has_up, has_dn))
    start(ccopy)
    start(kcopy)
    start(wcopy)

    load_mix.wait()
    for i in range(3):
        for j in range(3):
            wp[:, (3 * i + j) * ch:(3 * i + j + 1) * ch] = jnp.swapaxes(mix[i, j, :ch], 0, 1)
    past = [
        mix[i, j, ch + k * cp:ch + (k + 1) * cp] for i in range(3) for k in range(frames) for j in range(3)
    ]
    lead = ws.shape[1] - 9 * depth
    past.append(jnp.zeros((lead, ch), BF))
    past = jnp.concatenate(past, axis=0)
    for n in range(0, ws.shape[1], ch):
        ws[:, n:n + ch] = jnp.swapaxes(past[n:n + ch], 0, 1)
    wide = jnp.broadcast_to(bias_row[...][None, :], (ch, ch))
    eye = lax.broadcasted_iota(jnp.int32, (ch, ch), 0) == lax.broadcasted_iota(jnp.int32, (ch, ch), 1)
    bias = jnp.sum(jnp.where(eye, wide, 0.0), axis=1, keepdims=True)

    filled = []
    for k in range(frames):
        mine = []
        for j in range(3):
            step = dxs[k] + 1 - j
            lo = jnp.where(dxs[k] > 0, 0, w + step)
            hi = jnp.where(dxs[k] > 0, step, w)
            mine.append((lane >= lo) & (lane < hi))
        filled.append(mine)
        for y in range(h):
            row = red[k * h + y]
            for j in range(3):
                moved = pltpu.roll(row, (dxs[k] + 1 - j + w) & (w - 1), 1)
                if j != 1:
                    out = (lane == 0) & (c == 0) if j == 0 else (lane == w - 1) & (c == nc - 1)
                    moved = jnp.where(out, jnp.zeros_like(moved), moved)
                xs[(k * h + y) * 3 + j] = moved

    arrive(qcopy)

    def ends(near, lf_turn, rt_turn):
        lf = jnp.concatenate(
            [pltpu.roll(near[0], (2 * w - 2 * h * g - lf_turn) % w, 1) for g in range(4)], axis=0
        )
        rt = jnp.concatenate(
            [pltpu.roll(near[1], (2 * w - 2 * h * g - rt_turn) % w, 1) for g in range(4)], axis=0
        )
        return jnp.where((lane_c & 1) == 0, lf, rt)

    pk[...] = ends(qrecv, 0, 2)

    def shifter(dx):
        plus = dx > 0
        masks, kills = [], []
        for j in range(3):
            step = dx + 1 - j
            lo = jnp.where(plus, w - step, 0)
            hi = jnp.where(plus, w, -step)
            masks.append((lane >= lo) & (lane < hi))
            at = jnp.int32(-1)
            if j == 0:
                at = jnp.where(plus | (c > 0), at, -step)
            if j == 2:
                at = jnp.where(plus & (c == nc - 1), w - 1 - step, at)
            kills.append(lane == at)

        def unpack(at, q, tile):
            turn = (jnp.where(plus, w - REACH_X, 0) - pitch * q + w) & (w - 1)
            unp[at] = pltpu.roll(tile, turn, 1)

        def shift(at, row):
            far = unp[at]
            for j in range(3):
                near = row if j == 1 else jnp.where(kills[j], jnp.zeros_like(row), row)
                both = jnp.where(masks[j], far, near)
                xs[at * 3 + j] = pltpu.roll(both, (dx + 1 - j + w) & (w - 1), 1)

        return unpack, shift

    def halo(d):
        arrive([vcopy[d], wcopy[d], ccopy[2 * d], ccopy[2 * d + 1]])
        @pl.when((has_up, has_dn)[d])
        def _():
            for s in (0, 1):
                dx = off[1, (down, up)[d][s]]
                side = jnp.where(dx > 0, jnp.int32(0), jnp.int32(1))
                unpack, shift = shifter(dx)
                first = own + (2 * d + s) * reach
                for m in range(reach):
                    if m < PACK:
                        unpack(first + m, m, crecv[d][side, s])
                    else:
                        unpack(first + m, rest * s + m - PACK, crecv[d][side, 2])
                for m in range(reach):
                    shift(first + m, vrecv[d, s * reach + m])

    def widen(t, edge):
        mid = sp[pl.ds(t * pb + ch, ch)]
        sp[pl.ds(t * pb, ch)] = jnp.where(lane_c == 0, edge, pltpu.roll(mid, 1, 1))
        sp[pl.ds(t * pb + 2 * ch, ch)] = jnp.where(lane_c == w - 1, edge, pltpu.roll(mid, w - 1, 1))

    def present(p):
        y = 2 * p
        rhs = jnp.concatenate([sp[pl.ds(y * pb, 3 * pb)], sp[pl.ds((y + 1) * pb, 3 * pb)]], axis=1)
        acc[p] = jnp.dot(wp[...], rhs, preferred_element_type=F32)

    for t in range(1, h + 1):
        widen(t, pltpu.roll(pk[...], (w - 2 * (t - 1)) % w, 1) if t > 1 else pk[...])
    for p in range(1, h // 2 - 1):
        present(p)
    arrive(hcopy)
    for k in range(frames):
        base = -jnp.where(dxs[k] > 0, REACH_X, 0) + 2 * w
        for y in range(h):
            tile = hrecv[went_x[k], hslot[k] * tiles + y // PACK]
            for j in range(3):
                turn = (dxs[k] + 1 - j - pitch * (y % PACK) + base) & (w - 1)
                at = (k * h + y) * 3 + j
                xs[at] = jnp.where(filled[k][j], pltpu.roll(tile, turn, 1), xs[at])

    def window(y):
        rows = []
        for i in range(3):
            for k in range(frames):
                at = y + i - 1 - dys[k]
                at = jnp.where(
                    at < 0, own + vslot[k] * reach + reach + at,
                    jnp.where(at >= h, own + (2 + vslot[k]) * reach + at - h, k * h + at),
                )
                part = xs[pl.ds(at * 3, 3)].reshape(depth, w)
                if y == 0 and i == 0:
                    part = jnp.where(r == 0, jnp.zeros_like(part), part)
                if y == h - 1 and i == 2:
                    part = jnp.where(r == nr - 1, jnp.zeros_like(part), part)
                rows.append(part)
        rows.append(rows[0][:lead])
        return jnp.concatenate(rows, axis=0)

    def finish_pair(p):
        rhs = jnp.concatenate([window(2 * p), window(2 * p + 1)], axis=1)
        total = acc[p] + jnp.dot(ws[...], rhs, preferred_element_type=F32)
        total = jnp.maximum(total + bias, 0.0).astype(BF)
        out_ref[2 * p] = total[:, :w]
        out_ref[2 * p + 1] = total[:, w:]

    last = h // 2 - 1
    free = (h - reach - 1) // 2

    def edge_pair(d):
        arrive([pcopy[d], kcopy[2 * d], kcopy[2 * d + 1]])
        if d == 0:
            widen(0, ends(krecv.at[0], 2 * h - 2, 2 * h))
        else:
            widen(h + 1, ends(krecv.at[1], 0, 2))
        present(last * d)
        finish_pair(last * d)

    first_above = (r % 2 == 1) | (r == 0)

    @pl.when(first_above)
    def _():
        halo(0)
        for p in range(1, free):
            finish_pair(p)
        edge_pair(0)
        halo(1)
        for p in range(free, last):
            finish_pair(p)
        edge_pair(1)

    @pl.when(jnp.logical_not(first_above))
    def _():
        halo(1)
        for p in range(last + 1 - free, last):
            finish_pair(p)
        edge_pair(1)
        halo(0)
        for p in range(1, last + 1 - free):
            finish_pair(p)
        edge_pair(0)

    for copies in (hcopy, vcopy, wcopy, qcopy, pcopy, ccopy, kcopy):
        finish(copies)


def place(rows_ref, out_hbm, turned, sem):
    n = out_hbm.shape[0] // CHUNKS
    copies = []
    for g in range(CHUNKS):
        part = pl.ds(g * n, n)
        turned[part] = jnp.swapaxes(rows_ref[:, part], 0, 1)
        copies.append(pltpu.make_async_copy(turned.at[part], out_hbm.at[part], sem.at[g]))
        copies[-1].start()
    for copy in copies:
        copy.wait()


def body(nr, nc, current_frame, history_frames, offsets, compress_weight, mixer_weight, mixer_bias):
    frames, ch, h, w = history_frames.shape
    cp = compress_weight.shape[0]
    depth = frames * cp
    reach = h // 2 + 1
    rows = frames * h + 4 * reach
    tiles = -(-h // PACK)
    mix = mixer_weight.transpose(0, 1, 3, 2)
    anyspace = pl.BlockSpec(memory_space=pl.ANY)
    vmem = pl.BlockSpec(memory_space=pltpu.VMEM)
    joined = pl.pallas_call(
        functools.partial(kernel, nr, nc),
        out_shape=pltpu.VMEM((h, ch, w), BF),
        in_specs=[anyspace] * 6,
        out_specs=vmem,
        scratch_shapes=[
            pltpu.SMEM((2, frames), jnp.int32),
            pltpu.VMEM((cp, ch), BF),
            pltpu.VMEM((ch,), F32),
            pltpu.VMEM((frames, ch, h, w), BF),
            pltpu.VMEM((ch, h, w), BF),
            pltpu.VMEM(mix.shape, BF),
            pltpu.VMEM((frames * h, cp, w), BF),
            pltpu.VMEM((2, 2 * reach, cp, w), BF),
            pltpu.VMEM((2, 2 * reach, cp, w), BF),
            pltpu.VMEM((frames * tiles, cp, w), BF),
            pltpu.VMEM((2, 2 * tiles, cp, w), BF),
            pltpu.VMEM((2, 2 * tiles, cp, w), BF),
            pltpu.VMEM((2, 3, cp, w), BF),
            pltpu.VMEM((2, 3, cp, w), BF),
            pltpu.VMEM((2, 3, cp, w), BF),
            pltpu.VMEM((ch, w), BF),
            pltpu.VMEM((ch // 4, w), BF),
            pltpu.VMEM((2, ch // 4, w), BF),
            pltpu.VMEM((2, 2, ch // 4, w), BF),
            pltpu.VMEM((ch, w), BF),
            pltpu.VMEM(((h + 2) * 3 * ch, w), BF),
            pltpu.VMEM((rows, cp, w), BF),
            pltpu.VMEM((rows * 3, cp, w), BF),
            pltpu.VMEM((h // 2, ch, 2 * w), F32),
            pltpu.VMEM((ch, 9 * ch), BF),
            pltpu.VMEM((ch, -(-9 * depth // 128) * 128), BF),
            pltpu.SemaphoreType.DMA((frames + 5,)),
            pltpu.SemaphoreType.DMA((7, 4)),
            pltpu.SemaphoreType.DMA((7, 4)),
            pltpu.SemaphoreType.REGULAR,
        ],
        compiler_params=pltpu.CompilerParams(collective_id=0, has_side_effects=True),
        name="join",
    )(offsets.T, history_frames, current_frame, mix, compress_weight, mixer_bias)
    return pl.pallas_call(
        place,
        out_shape=jax.ShapeDtypeStruct((ch, h, w), BF),
        in_specs=[vmem],
        out_specs=anyspace,
        scratch_shapes=[pltpu.VMEM((ch, h, w), BF), pltpu.SemaphoreType.DMA((CHUNKS,))],
        name="place",
    )(pltpu.with_memory_space_constraint(joined, pltpu.VMEM))


def solution(mesh):
    in_specs = (P(None, "rows", "cols"), P(None, None, "rows", "cols"), P(), P(), P(), P())
    out_specs = P(None, "rows", "cols")
    return jax.shard_map(
        functools.partial(body, mesh.shape["rows"], mesh.shape["cols"]),
        mesh=mesh, in_specs=in_specs, out_specs=out_specs, check_vma=False,
    )
```

```python
import functools

import jax
import jax.numpy as jnp
from jax import lax
from jax.experimental import pallas as pl
from jax.experimental.pallas import tpu as pltpu
from jax.sharding import PartitionSpec as P

MESH = pl.DeviceIdType.MESH
BF = jnp.bfloat16
F32 = jnp.float32
PACK = 7
CHUNKS = 4
REACH_X = 17


def pick(ds, positive):
    n = len(ds)
    first, last = jnp.int32(n - 1), jnp.int32(0)
    for k in range(n):
        hit = ds[k] > 0 if positive else ds[k] < 0
        last = jnp.where(hit, jnp.int32(k), last)
    for k in reversed(range(n)):
        hit = ds[k] > 0 if positive else ds[k] < 0
        first = jnp.where(hit, jnp.int32(k), first)
    return first, last


def kernel(
    nr, nc,
    off_hbm, hist_hbm, cur_hbm, mix_hbm, cw_hbm, bias_hbm, out_ref,
    off, cw, bias_row, hist, cur, mix, red, vsend, vrecv, packs, hsend, hrecv, csend, crecv_a, crecv_b,
    qfull, qsend, qrecv, krecv, pk, sp, unp, xs, acc, wp, ws, lsem, ssem, rsem, ready,
):
    frames, ch, h, w = hist.shape
    cp = cw.shape[0]
    depth = frames * cp
    reach = h // 2 + 1
    pitch = w // PACK
    tiles = -(-h // PACK)
    rest = reach - PACK
    own = frames * h
    pb = 3 * ch
    quarter = ch // 4

    r = lax.axis_index("rows")
    c = lax.axis_index("cols")
    has_up, has_dn, has_lf, has_rt = r > 0, r < nr - 1, c > 0, c < nc - 1
    above, below = (r - 1, has_up), (r + 1, has_dn)
    before, after = (c - 1, has_lf), (c + 1, has_rt)

    barrier = pltpu.get_barrier_semaphore()
    near = ((r - 1, c, has_up), (r + 1, c, has_dn), (r, c - 1, has_lf), (r, c + 1, has_rt))
    for rr, cc, cond in near:
        @pl.when(cond)
        def _(dev=(rr, cc)):
            pl.semaphore_signal(barrier, inc=1, device_id=dev, device_id_type=MESH)

    small = [
        pltpu.make_async_copy(src, dst, lsem.at[n])
        for n, (src, dst) in enumerate(((off_hbm, off), (cw_hbm, cw), (bias_hbm, bias_row)))
    ]
    loads = [pltpu.make_async_copy(hist_hbm.at[k], hist.at[k], lsem.at[3 + k]) for k in range(frames)]
    load_cur = pltpu.make_async_copy(cur_hbm, cur, lsem.at[3 + frames])
    load_mix = pltpu.make_async_copy(mix_hbm, mix, lsem.at[4 + frames])
    for x in (load_cur, *loads, *small, load_mix):
        x.start()

    def number(*conds):
        return sum(jnp.where(x, jnp.int32(1), jnp.int32(0)) for x in conds)

    def remote(n, src, dst, dv=None, dh=None):
        rr, sends, comes, m = r, True, True, 0
        cc = c
        if dv is not None:
            (rr, sends), (_, comes) = (below, above) if dv == 0 else (above, below)
            m = dv
        if dh is not None:
            (cc, out), (_, into) = (after, before) if dh == 0 else (before, after)
            sends, comes = sends & out, comes & into
            m = 2 * m + dh if dv is not None else dh
        copy = pltpu.make_async_remote_copy(
            src_ref=src, dst_ref=dst, send_sem=ssem.at[n, m], recv_sem=rsem.at[n, m],
            device_id=(rr, cc), device_id_type=MESH,
        )
        return copy, sends, comes

    def start(copies):
        for copy, sends, _ in copies:
            @pl.when(sends)
            def _(copy=copy):
                copy.start()

    def arrive(copies):
        for copy, _, comes in copies:
            @pl.when(comes)
            def _(copy=copy):
                copy.wait_recv()

    def finish(copies):
        for copy, sends, _ in copies:
            @pl.when(sends)
            def _(copy=copy):
                copy.wait_send()

    hcopy = [remote(0, hsend.at[d], hrecv.at[d], dh=d) for d in (0, 1)]
    def vpart(n, s):
        part = pl.ds(s * reach, reach)
        return [remote(n, vsend.at[d, part], vrecv.at[d, part], dv=d) for d in (0, 1)]

    vcopy, wcopy = vpart(1, 0), vpart(6, 1)
    qcopy = [remote(2, qsend, qrecv.at[d], dh=d) for d in (0, 1)]
    pcopy = [
        remote(3, sp.at[pl.ds(h * pb + ch, ch)], sp.at[pl.ds(ch, ch)], dv=0),
        remote(3, sp.at[pl.ds(pb + ch, ch)], sp.at[pl.ds((h + 1) * pb + ch, ch)], dv=1),
    ]
    crecv = (crecv_a, crecv_b)
    corners = [(dv, dh) for dv in (0, 1) for dh in (0, 1)]
    ccopy = [remote(4, csend.at[dv], crecv[dv].at[dh], dv, dh) for dv, dh in corners]
    kcopy = [remote(5, qsend, krecv.at[dv, dh], dv, dh) for dv, dh in corners]

    def clear(ref):
        ref[...] = jnp.zeros(ref.shape, BF)

    @pl.when(r == 0)
    def _():
        for ref in (xs.at[pl.ds(own * 3, 6 * reach)], krecv.at[0], sp.at[pl.ds(ch, ch)]):
            clear(ref)

    @pl.when(r == nr - 1)
    def _():
        for ref in (xs.at[pl.ds((own + 2 * reach) * 3, 6 * reach)], krecv.at[1], sp.at[pl.ds((h + 1) * pb + ch, ch)]):
            clear(ref)

    @pl.when(c == 0)
    def _():
        for ref in (hrecv.at[0], qrecv.at[0], crecv[0].at[0], crecv[1].at[0], krecv.at[0, 0], krecv.at[1, 0]):
            clear(ref)

    @pl.when(c == nc - 1)
    def _():
        for ref in (hrecv.at[1], qrecv.at[1], crecv[0].at[1], crecv[1].at[1], krecv.at[0, 1], krecv.at[1, 1]):
            clear(ref)

    for x in small:
        x.wait()
    dys = [off[0, k] for k in range(frames)]
    dxs = [off[1, k] for k in range(frames)]
    down, up = pick(dys, True), pick(dys, False)
    right, left = pick(dxs, True), pick(dxs, False)

    def slot(k, d, plus, minus):
        other = jnp.where(d > 0, plus[0], minus[0]) != k
        return jnp.where(other, jnp.int32(1), jnp.int32(0))

    vslot = [slot(k, dys[k], down, up) for k in range(frames)]
    hslot = [slot(k, dxs[k], right, left) for k in range(frames)]
    went_x = [jnp.where(dxs[k] > 0, jnp.int32(0), jnp.int32(1)) for k in range(frames)]
    went_y = [jnp.where(dys[k] > 0, jnp.int32(0), jnp.int32(1)) for k in range(frames)]

    load_cur.wait()
    rows = jnp.swapaxes(cur[...], 0, 1)
    for y in range(h):
        sp[pl.ds((y + 1) * pb + ch, ch)] = rows[y]
    lane_c = lax.broadcasted_iota(jnp.int32, (ch, w), 1)
    tile = jnp.zeros((ch, w), BF)
    for y in range(h):
        turned = pltpu.roll(rows[y], 2 * y + 1, 1)
        tile = jnp.where((lane_c == 2 * y) | (lane_c == 2 * y + 1), turned, tile)
    qfull[...] = tile
    small = qfull[pl.ds(0, quarter)]
    lane_q = lax.broadcasted_iota(jnp.int32, (quarter, w), 1)
    for g in range(1, 4):
        turned = pltpu.roll(qfull[pl.ds(g * quarter, quarter)], 2 * h * g, 1)
        small = jnp.where(lane_q >= 2 * h * g, turned, small)
    qsend[...] = small

    for k in range(frames):
        if k == 2:
            pl.semaphore_wait(barrier, number(has_up, has_dn, has_lf, has_rt))
            for rr, cc, cond in near[:2]:
                @pl.when(cond)
                def _(dev=(rr, cc)):
                    pl.semaphore_signal(ready, inc=1, device_id=dev, device_id_type=MESH)
            start(qcopy)
            start(pcopy)
        loads[k].wait()
        rows = jnp.swapaxes(hist[k], 0, 1)
        for y in range(0, h, 2):
            rhs = jnp.concatenate([rows[y], rows[y + 1]], axis=1)
            got = jnp.dot(cw[...], rhs, preferred_element_type=F32).astype(BF)
            for e in (0, 1):
                red[k * h + y + e] = got[:, e * w:(e + 1) * w]

    @pl.when(r > 0)
    def _():
        for s in (0, 1):
            vsend[0, pl.ds(s * reach, reach)] = red[pl.ds(down[s] * h + h - reach, reach)]
            vsend[1, pl.ds(s * reach, reach)] = red[pl.ds(up[s] * h, reach)]
        start(vcopy)

    lane = lax.broadcasted_iota(jnp.int32, (cp, w), 1)
    for k in range(frames):
        for g in range(tiles):
            tile = None
            for q in range(min(PACK, h - PACK * g)):
                turn = jnp.where(dxs[k] > 0, jnp.int32((REACH_X + pitch * q) % w), jnp.int32(pitch * q))
                row = pltpu.roll(red[k * h + PACK * g + q], turn, 1)
                tile = row if tile is None else jnp.where(lane >= pitch * q, row, tile)
            packs[k * tiles + g] = tile
    for s in (0, 1):
        for d in (0, 1):
            frame = (right, left)[d][s]
            hsend[d, pl.ds(s * tiles, tiles)] = packs[pl.ds(frame * tiles, tiles)]
    start(hcopy)

    @pl.when(r == 0)
    def _():
        for s in (0, 1):
            vsend[0, pl.ds(s * reach, reach)] = red[pl.ds(down[s] * h + h - reach, reach)]
            vsend[1, pl.ds(s * reach, reach)] = red[pl.ds(up[s] * h, reach)]
        start(vcopy)


    for d in (0, 1):
        at = [(down, up)[d][s] * tiles + (1 if d == 0 else 0) for s in (0, 1)]
        for s in (0, 1):
            csend[d, s] = packs[at[s]]
        turned = pltpu.roll(packs[at[1] + 1], rest * pitch, 1)
        csend[d, 2] = jnp.where(lane < rest * pitch, packs[at[0] + 1], turned)
    pl.semaphore_wait(ready, number(has_up, has_dn))
    start(ccopy)
    start(kcopy)
    start(wcopy)

    load_mix.wait()
    for i in range(3):
        for j in range(3):
            wp[:, (3 * i + j) * ch:(3 * i + j + 1) * ch] = jnp.swapaxes(mix[i, j, :ch], 0, 1)
    past = [
        mix[i, j, ch + k * cp:ch + (k + 1) * cp] for i in range(3) for k in range(frames) for j in range(3)
    ]
    lead = ws.shape[1] - 9 * depth
    past.append(jnp.zeros((lead, ch), BF))
    past = jnp.concatenate(past, axis=0)
    for n in range(0, ws.shape[1], ch):
        ws[:, n:n + ch] = jnp.swapaxes(past[n:n + ch], 0, 1)
    wide = jnp.broadcast_to(bias_row[...][None, :], (ch, ch))
    eye = lax.broadcasted_iota(jnp.int32, (ch, ch), 0) == lax.broadcasted_iota(jnp.int32, (ch, ch), 1)
    bias = jnp.sum(jnp.where(eye, wide, 0.0), axis=1, keepdims=True)

    filled = []
    for k in range(frames):
        mine = []
        for j in range(3):
            step = dxs[k] + 1 - j
            lo = jnp.where(dxs[k] > 0, 0, w + step)
            hi = jnp.where(dxs[k] > 0, step, w)
            mine.append((lane >= lo) & (lane < hi))
        filled.append(mine)
        for y in range(h):
            row = red[k * h + y]
            for j in range(3):
                moved = pltpu.roll(row, (dxs[k] + 1 - j + w) & (w - 1), 1)
                if j != 1:
                    out = (lane == 0) & (c == 0) if j == 0 else (lane == w - 1) & (c == nc - 1)
                    moved = jnp.where(out, jnp.zeros_like(moved), moved)
                xs[(k * h + y) * 3 + j] = moved

    arrive(qcopy)

    def ends(near, lf_turn, rt_turn):
        lf = jnp.concatenate(
            [pltpu.roll(near[0], (2 * w - 2 * h * g - lf_turn) % w, 1) for g in range(4)], axis=0
        )
        rt = jnp.concatenate(
            [pltpu.roll(near[1], (2 * w - 2 * h * g - rt_turn) % w, 1) for g in range(4)], axis=0
        )
        return jnp.where((lane_c & 1) == 0, lf, rt)

    pk[...] = ends(qrecv, 0, 2)

    def shifter(dx):
        plus = dx > 0
        masks, kills = [], []
        for j in range(3):
            step = dx + 1 - j
            lo = jnp.where(plus, w - step, 0)
            hi = jnp.where(plus, w, -step)
            masks.append((lane >= lo) & (lane < hi))
            at = jnp.int32(-1)
            if j == 0:
                at = jnp.where(plus | (c > 0), at, -step)
            if j == 2:
                at = jnp.where(plus & (c == nc - 1), w - 1 - step, at)
            kills.append(lane == at)

        def unpack(at, q, tile):
            turn = (jnp.where(plus, w - REACH_X, 0) - pitch * q + w) & (w - 1)
            unp[at] = pltpu.roll(tile, turn, 1)

        def shift(at, row):
            far = unp[at]
            for j in range(3):
                near = row if j == 1 else jnp.where(kills[j], jnp.zeros_like(row), row)
                both = jnp.where(masks[j], far, near)
                xs[at * 3 + j] = pltpu.roll(both, (dx + 1 - j + w) & (w - 1), 1)

        return unpack, shift

    def halo(d):
        arrive([vcopy[d], wcopy[d], ccopy[2 * d], ccopy[2 * d + 1]])
        @pl.when((has_up, has_dn)[d])
        def _():
            for s in (0, 1):
                dx = off[1, (down, up)[d][s]]
                side = jnp.where(dx > 0, jnp.int32(0), jnp.int32(1))
                unpack, shift = shifter(dx)
                first = own + (2 * d + s) * reach
                for m in range(reach):
                    if m < PACK:
                        unpack(first + m, m, crecv[d][side, s])
                    else:
                        unpack(first + m, rest * s + m - PACK, crecv[d][side, 2])
                for m in range(reach):
                    shift(first + m, vrecv[d, s * reach + m])

    def widen(t, edge):
        mid = sp[pl.ds(t * pb + ch, ch)]
        sp[pl.ds(t * pb, ch)] = jnp.where(lane_c == 0, edge, pltpu.roll(mid, 1, 1))
        sp[pl.ds(t * pb + 2 * ch, ch)] = jnp.where(lane_c == w - 1, edge, pltpu.roll(mid, w - 1, 1))

    def present(p):
        y = 2 * p
        rhs = jnp.concatenate([sp[pl.ds(y * pb, 3 * pb)], sp[pl.ds((y + 1) * pb, 3 * pb)]], axis=1)
        acc[p] = jnp.dot(wp[...], rhs, preferred_element_type=F32)

    for t in range(1, h + 1):
        widen(t, pltpu.roll(pk[...], (w - 2 * (t - 1)) % w, 1) if t > 1 else pk[...])
    for p in range(1, h // 2 - 1):
        present(p)
    arrive(hcopy)
    for k in range(frames):
        base = -jnp.where(dxs[k] > 0, REACH_X, 0) + 2 * w
        for y in range(h):
            tile = hrecv[went_x[k], hslot[k] * tiles + y // PACK]
            for j in range(3):
                turn = (dxs[k] + 1 - j - pitch * (y % PACK) + base) & (w - 1)
                at = (k * h + y) * 3 + j
                xs[at] = jnp.where(filled[k][j], pltpu.roll(tile, turn, 1), xs[at])

    def window(y):
        rows = []
        for i in range(3):
            for k in range(frames):
                at = y + i - 1 - dys[k]
                at = jnp.where(
                    at < 0, own + vslot[k] * reach + reach + at,
                    jnp.where(at >= h, own + (2 + vslot[k]) * reach + at - h, k * h + at),
                )
                part = xs[pl.ds(at * 3, 3)].reshape(depth, w)
                if y == 0 and i == 0:
                    part = jnp.where(r == 0, jnp.zeros_like(part), part)
                if y == h - 1 and i == 2:
                    part = jnp.where(r == nr - 1, jnp.zeros_like(part), part)
                rows.append(part)
        rows.append(rows[0][:lead])
        return jnp.concatenate(rows, axis=0)

    def finish_pair(p):
        rhs = jnp.concatenate([window(2 * p), window(2 * p + 1)], axis=1)
        total = acc[p] + jnp.dot(ws[...], rhs, preferred_element_type=F32)
        total = jnp.maximum(total + bias, 0.0).astype(BF)
        out_ref[2 * p] = total[:, :w]
        out_ref[2 * p + 1] = total[:, w:]

    last = h // 2 - 1
    free = (h - reach - 1) // 2

    def edge_pair(d):
        arrive([pcopy[d], kcopy[2 * d], kcopy[2 * d + 1]])
        if d == 0:
            widen(0, ends(krecv.at[0], 2 * h - 2, 2 * h))
        else:
            widen(h + 1, ends(krecv.at[1], 0, 2))
        present(last * d)
        finish_pair(last * d)

    first_above = (r % 2 == 1) | (r == 0)

    @pl.when(first_above)
    def _():
        halo(0)
        for p in range(1, free):
            finish_pair(p)
        edge_pair(0)
        halo(1)
        for p in range(free, last):
            finish_pair(p)
        edge_pair(1)

    @pl.when(jnp.logical_not(first_above))
    def _():
        halo(1)
        for p in range(last + 1 - free, last):
            finish_pair(p)
        edge_pair(1)
        halo(0)
        for p in range(1, last + 1 - free):
            finish_pair(p)
        edge_pair(0)

    for copies in (hcopy, vcopy, wcopy, qcopy, pcopy, ccopy, kcopy):
        finish(copies)


def place(rows_ref, out_hbm, turned, sem):
    n = out_hbm.shape[0] // CHUNKS
    copies = []
    for g in range(CHUNKS):
        part = pl.ds(g * n, n)
        turned[part] = jnp.swapaxes(rows_ref[:, part], 0, 1)
        copies.append(pltpu.make_async_copy(turned.at[part], out_hbm.at[part], sem.at[g]))
        copies[-1].start()
    for copy in copies:
        copy.wait()


def body(nr, nc, current_frame, history_frames, offsets, compress_weight, mixer_weight, mixer_bias):
    frames, ch, h, w = history_frames.shape
    cp = compress_weight.shape[0]
    depth = frames * cp
    reach = h // 2 + 1
    rows = frames * h + 4 * reach
    tiles = -(-h // PACK)
    mix = mixer_weight.transpose(0, 1, 3, 2)
    anyspace = pl.BlockSpec(memory_space=pl.ANY)
    vmem = pl.BlockSpec(memory_space=pltpu.VMEM)
    joined = pl.pallas_call(
        functools.partial(kernel, nr, nc),
        out_shape=pltpu.VMEM((h, ch, w), BF),
        in_specs=[anyspace] * 6,
        out_specs=vmem,
        scratch_shapes=[
            pltpu.SMEM((2, frames), jnp.int32),
            pltpu.VMEM((cp, ch), BF),
            pltpu.VMEM((ch,), F32),
            pltpu.VMEM((frames, ch, h, w), BF),
            pltpu.VMEM((ch, h, w), BF),
            pltpu.VMEM(mix.shape, BF),
            pltpu.VMEM((frames * h, cp, w), BF),
            pltpu.VMEM((2, 2 * reach, cp, w), BF),
            pltpu.VMEM((2, 2 * reach, cp, w), BF),
            pltpu.VMEM((frames * tiles, cp, w), BF),
            pltpu.VMEM((2, 2 * tiles, cp, w), BF),
            pltpu.VMEM((2, 2 * tiles, cp, w), BF),
            pltpu.VMEM((2, 3, cp, w), BF),
            pltpu.VMEM((2, 3, cp, w), BF),
            pltpu.VMEM((2, 3, cp, w), BF),
            pltpu.VMEM((ch, w), BF),
            pltpu.VMEM((ch // 4, w), BF),
            pltpu.VMEM((2, ch // 4, w), BF),
            pltpu.VMEM((2, 2, ch // 4, w), BF),
            pltpu.VMEM((ch, w), BF),
            pltpu.VMEM(((h + 2) * 3 * ch, w), BF),
            pltpu.VMEM((rows, cp, w), BF),
            pltpu.VMEM((rows * 3, cp, w), BF),
            pltpu.VMEM((h // 2, ch, 2 * w), F32),
            pltpu.VMEM((ch, 9 * ch), BF),
            pltpu.VMEM((ch, -(-9 * depth // 128) * 128), BF),
            pltpu.SemaphoreType.DMA((frames + 5,)),
            pltpu.SemaphoreType.DMA((7, 4)),
            pltpu.SemaphoreType.DMA((7, 4)),
            pltpu.SemaphoreType.REGULAR,
        ],
        compiler_params=pltpu.CompilerParams(collective_id=0, has_side_effects=True),
        name="join",
    )(offsets.T, history_frames, current_frame, mix, compress_weight, mixer_bias)
    return pl.pallas_call(
        place,
        out_shape=jax.ShapeDtypeStruct((ch, h, w), BF),
        in_specs=[vmem],
        out_specs=anyspace,
        scratch_shapes=[pltpu.VMEM((ch, h, w), BF), pltpu.SemaphoreType.DMA((CHUNKS,))],
        name="place",
    )(pltpu.with_memory_space_constraint(joined, pltpu.VMEM))


def solution(mesh):
    in_specs = (P(None, "rows", "cols"), P(None, None, "rows", "cols"), P(), P(), P(), P())
    out_specs = P(None, "rows", "cols")
    return jax.shard_map(
        functools.partial(body, mesh.shape["rows"], mesh.shape["cols"]),
        mesh=mesh, in_specs=in_specs, out_specs=out_specs, check_vma=False,
    )
```
